32 devices in a mesh: rack: 4 (over x, core), chip: 8 (over z, y).
Axes of the slice: x: 2, y: 2, z: 4, core: 2. Of those that a mesh axis runs over, the one named last changes fastest.
Arguments:
- points: float32 [64, 4, 32, 256], P(('rack', 'chip')), may hold values from -6 to 6
- counts: int32 [64, 256], P(('rack', 'chip')), may hold values from 1 to 32
- cells: int32 [64, 256], P(('rack', 'chip')), may hold values from 0 to 2047, as said below
- pfn_weight: float32 [9, 64], replicated, may hold values from -2 to 2
- pfn_gain: float32 [64], replicated, may hold values from 0.5 to 1.5
- pfn_bias: float32 [64], replicated, may hold values from -3 to 3
- conv_weight: float32 [4, 9, 4096], replicated, may hold values from -0.25 to 0.25
- bn_gain: float32 [4, 64], replicated, may hold values from 0.5 to 1.5
- bn_bias: float32 [4, 64], replicated, may hold values from -3 to 3
- cotangent: float32 [64, 64, 4, 128], P(('rack', 'chip')), may hold values from -0.006 to 0.006
Outputs:
- features: float32 [64, 64, 4, 128], P(('rack', 'chip'))
- conv_grads: float32 [4, 9, 4096], replicated
- norm_grads: float32 [2, 4, 64], replicated
- pillar_grad: float32 [64, 64, 256], P(('rack', 'chip'))
The draws below stay inside these ranges and needn't reach their ends.
Inputs may be any that keep to these rules, and one draw needn't show every extreme that they name: `cells`: within one sweep no two pillars share a cell.
All inputs are finite; a program needn't handle non-finite values.
Results may differ from the reference program's by a relative error of at most 0.0003.
Values sent between devices are 32-bit elements; how exact they have to be, the bound alone decides.
A program may use at most 128 MiB of HBM per device.

```python
import jax
import jax.numpy as jnp
from jax import lax

C = 64
MAXP = 32
LAYERS = 4
GH = 8
GW = 256
PILL = 256
SWEEPS = 64


def draw_cells(key, part):
    keys = jax.random.split(key, SWEEPS)

    def one_sweep(sweep_key):
        return jax.random.permutation(sweep_key, GH * GW)[:PILL].astype(jnp.int32)
    return jax.vmap(one_sweep)(keys)


def touch_ends(values, own_key, least, largest):
    dims = values.shape
    spot = [jax.random.randint(jax.random.fold_in(own_key, axis), (), 0, dims[axis]) for axis in range(len(dims))]
    values = values.at[tuple(spot)].set(least)
    longest = dims.index(max(dims))
    spot[longest] = (spot[longest] + 1) % dims[longest]
    return values.at[tuple(spot)].set(largest)


def steps_of(rng, dims, pieces, smallest, largest):
    def one(axis_at, shards_of):
        heights = jax.random.uniform(jax.random.fold_in(jax.random.fold_in(rng, 6), axis_at), (shards_of,), jnp.float32, smallest / len(pieces), largest / len(pieces))
        return jnp.repeat(jnp.exp(heights), dims[axis_at] // shards_of).reshape((-1,) + (1,) * (len(dims) - axis_at - 1))

    level = one(*pieces[0])
    for cut in pieces[1:]:
        level = level * one(*cut)
    return level


def bell_draw(own_key, shape, spread, bound, pieces=(), kind=jnp.bfloat16):
    values = jax.random.normal(own_key, shape, jnp.float32) * spread
    if len(pieces) > 0:
        values = steps_of(own_key, shape, pieces, -0.22, 0.18) * values
    return jnp.clip(values, min=-bound, max=bound).astype(kind)


def setup_inputs(seed: int = 0) -> dict:
    streams_of = jax.random.split(jax.random.key(seed), 11)
    points = bell_draw(streams_of[0], (SWEEPS, 4, MAXP, PILL), 1.0, 6.0, ((0, 32),), jnp.float32)
    counts = touch_ends(jax.random.randint(streams_of[1], (SWEEPS, PILL), 1, MAXP + 1), jax.random.fold_in(streams_of[1], 1), 1, MAXP).astype(jnp.int32)
    cells = draw_cells(jax.random.fold_in(streams_of[10], 71), 0)
    pfn_weight = bell_draw(streams_of[3], (9, C), 9 ** -0.5, 2.0, (), jnp.float32)
    pfn_gain = jnp.clip(1.0 + 0.1 * jax.random.normal(streams_of[4], (C,), jnp.float32), 0.5, 1.5)
    pfn_bias = bell_draw(streams_of[5], (C,), 0.5, 3.0, (), jnp.float32)
    conv_weight = bell_draw(streams_of[6], (LAYERS, 9, C * C), (9 * C) ** -0.5, 0.25, (), jnp.float32)
    bn_gain = jnp.clip(1.0 + 0.1 * jax.random.normal(streams_of[7], (LAYERS, C), jnp.float32), 0.5, 1.5)
    bn_bias = bell_draw(streams_of[8], (LAYERS, C), 0.5, 3.0, (), jnp.float32)
    cotangent = bell_draw(streams_of[9], (SWEEPS, C, GH // 2, GW // 2), 0.001, 0.006, ((0, 32),), jnp.float32)
    return dict(points=points, counts=counts, cells=cells, pfn_weight=pfn_weight, pfn_gain=pfn_gain, pfn_bias=pfn_bias, conv_weight=conv_weight, bn_gain=bn_gain, bn_bias=bn_bias, cotangent=cotangent)


EPS = 1e-05
PRECISE = lax.Precision.HIGHEST

def channel_shape(vector, ndim):
    return vector.reshape((1, -1) + (1,) * (ndim - 2))

def silu_slope(pre_act):
    sigma = jax.nn.sigmoid(pre_act)
    return sigma * (1.0 + pre_act * (1.0 - sigma))

def pillar_hidden(points, counts, cells, pfn_weight):
    slot_ids = lax.broadcasted_iota(jnp.int32, (1, points.shape[2], 1), 1)
    is_valid = (slot_ids < counts[:, None, :]).astype(jnp.float32)
    point_count = counts.astype(jnp.float32)
    centroid = lax.optimization_barrier(jnp.sum(points[:, 0:3] * is_valid[:, None], axis=2)) / point_count[:, None]
    col_pos = (cells % GW).astype(jnp.float32) * (2.0 / GW) - 1.0
    row_pos = (cells // GW).astype(jnp.float32) * (2.0 / GH) - 1.0
    offsets = points[:, 0:3] - centroid[:, :, None, :]
    grid_off = jnp.stack([points[:, 0] - col_pos[:, None, :], points[:, 1] - row_pos[:, None, :]], axis=1)
    inputs = jnp.concatenate([points, offsets, grid_off], axis=1)
    hidden = jnp.einsum('fc,sfpq->scpq', pfn_weight, inputs, precision=PRECISE)
    return (hidden, is_valid)

def normalize_pillars(hidden, is_valid, mean_val, inv_std, gain, bias):
    scaled = channel_shape(gain, 4) * (hidden - channel_shape(mean_val, 4)) * channel_shape(inv_std, 4) + channel_shape(bias, 4)
    return lax.optimization_barrier(jnp.max(jnp.maximum(scaled, 0.0) * is_valid[:, None], axis=2))

def scatter_pillars(pillar, cells):
    empty = jnp.zeros((pillar.shape[1], GH * GW), pillar.dtype)
    placed = jax.vmap(lambda feature, target: empty.at[:, target].set(feature))(pillar, cells)
    return placed.reshape(pillar.shape[0], pillar.shape[1], GH, GW)

def conv_forward(activation, taps, stride):
    padded = jnp.pad(activation, ((0, 0), (0, 0), (1, 1), (1, 1)))
    height = activation.shape[2] // stride
    width = activation.shape[3] // stride
    result = jnp.zeros((activation.shape[0], C, height, width), jnp.float32)
    for row_tap in range(3):
        for col_tap in range(3):
            tap_slice = padded[:, :, row_tap:row_tap + stride * height:stride, col_tap:col_tap + stride * width:stride]
            kernel = taps[3 * row_tap + col_tap].reshape(C, C)
            result = result + jnp.einsum('oi,nihw->nohw', kernel, tap_slice, precision=PRECISE)
    return result

def conv_backward(activation, taps, grad_z, stride):
    padded = jnp.pad(activation, ((0, 0), (0, 0), (1, 1), (1, 1)))
    height = grad_z.shape[2]
    width = grad_z.shape[3]
    grad_pad = jnp.zeros(padded.shape, jnp.float32)
    tap_grads = []
    for row_tap in range(3):
        for col_tap in range(3):
            tap_slice = padded[:, :, row_tap:row_tap + stride * height:stride, col_tap:col_tap + stride * width:stride]
            tap_grads.append(jnp.einsum('nohw,nihw->oi', grad_z, tap_slice, precision=PRECISE).reshape(C * C))
            kernel = taps[3 * row_tap + col_tap].reshape(C, C)
            back = jnp.einsum('oi,nohw->nihw', kernel, grad_z, precision=PRECISE)
            grad_pad = grad_pad.at[:, :, row_tap:row_tap + stride * height:stride, col_tap:col_tap + stride * width:stride].add(back)
    return (jnp.stack(tap_grads), grad_pad[:, :, 1:-1, 1:-1])

def reference(points, counts, cells, pfn_weight, pfn_gain, pfn_bias, conv_weight, bn_gain, bn_bias, cotangent):

    def hidden_of(args):
        return pillar_hidden(args[0][None], args[1][None], args[2][None], pfn_weight)

    def first_sums(args):
        hidden, is_valid = hidden_of(args)
        return (lax.optimization_barrier(jnp.sum(hidden * is_valid[:, None], axis=(0, 2, 3))), jnp.sum(is_valid))
    totals, counts_each = lax.map(first_sums, (points, counts, cells))
    count_all = jnp.sum(counts_each)
    mean_val = lax.optimization_barrier(jnp.sum(totals, axis=0)) / count_all

    def second_sums(args):
        hidden, is_valid = hidden_of(args)
        centred = hidden - channel_shape(mean_val, 4)
        return lax.optimization_barrier(jnp.sum(centred * centred * is_valid[:, None], axis=(0, 2, 3)))
    variance = lax.optimization_barrier(jnp.sum(lax.map(second_sums, (points, counts, cells)), axis=0)) / count_all
    inv_std = lax.rsqrt(variance + EPS)

    def to_grid(args):
        hidden, is_valid = hidden_of(args)
        pillar = normalize_pillars(hidden, is_valid, mean_val, inv_std, pfn_gain, pfn_bias)
        return scatter_pillars(pillar, args[2][None])[0]
    bev_grid = lax.map(to_grid, (points, counts, cells))
    activations = [bev_grid]
    normals = []
    for layer_idx in range(LAYERS):
        stride = 2 if layer_idx == 0 else 1
        weight = conv_weight[layer_idx]
        pre_norm = lax.map(lambda sweep: conv_forward(sweep[None], weight, stride)[0], activations[-1])
        mean_c = lax.optimization_barrier(jnp.mean(pre_norm, axis=(0, 2, 3)))
        centred = pre_norm - channel_shape(mean_c, 4)
        inv_c = lax.rsqrt(lax.optimization_barrier(jnp.mean(centred * centred, axis=(0, 2, 3))) + EPS)
        normed = centred * channel_shape(inv_c, 4)
        scaled = channel_shape(bn_gain[layer_idx], 4) * normed + channel_shape(bn_bias[layer_idx], 4)
        activations.append(jax.nn.silu(scaled))
        normals.append((normed, inv_c, scaled))
    upstream = cotangent
    grad_list = [None] * LAYERS
    gain_list = [None] * LAYERS
    bias_list = [None] * LAYERS
    pillar_grad = None
    for layer_idx in range(LAYERS - 1, -1, -1):
        stride = 2 if layer_idx == 0 else 1
        weight = conv_weight[layer_idx]
        normed, inv_c, scaled = normals[layer_idx]
        grad_y = upstream * silu_slope(scaled)
        sum_dy = lax.optimization_barrier(jnp.sum(grad_y, axis=(0, 2, 3)))
        sum_dyx = lax.optimization_barrier(jnp.sum(grad_y * normed, axis=(0, 2, 3)))
        entries = float(grad_y.shape[0] * grad_y.shape[2] * grad_y.shape[3])
        grad_z = channel_shape(bn_gain[layer_idx] * inv_c, 4) * (grad_y - channel_shape(sum_dy / entries, 4) - normed * channel_shape(sum_dyx / entries, 4))
        if layer_idx == 0:

            def back_first(args):
                grad_w, grad_in = conv_backward(args[0][None], weight, args[1][None], stride)
                plane = grad_in[0].reshape(grad_in.shape[1], GH * GW)
                return (grad_w, plane[:, args[2]])
            parts, pillar_grad = lax.map(back_first, (activations[0], grad_z, cells))
        else:

            def back_other(args):
                grad_w, grad_in = conv_backward(args[0][None], weight, args[1][None], stride)
                return (grad_w, grad_in[0])
            parts, upstream = lax.map(back_other, (activations[layer_idx], grad_z))
        grad_list[layer_idx] = lax.optimization_barrier(jnp.sum(parts, axis=0))
        gain_list[layer_idx] = sum_dyx
        bias_list[layer_idx] = sum_dy
    norm_grads = jnp.stack([jnp.stack(gain_list), jnp.stack(bias_list)])
    return (activations[-1], jnp.stack(grad_list), norm_grads, pillar_grad)
```

```python
import functools

import jax
import jax.numpy as jnp
from jax import lax
from jax.experimental import pallas as pl
from jax.experimental.pallas import tpu as pltpu
from jax.sharding import PartitionSpec as P

LAYERS = 4
LINEAR = (0, 1)
EPS = 1e-05
F32 = jnp.float32
BF16 = jnp.bfloat16
NN = (((1,), (0,)), ((), ()))
NT = (((1,), (1,)), ((), ()))
LOWEST = -3e38


class Peer:
    def __init__(self, rack, chip, index):
        self.rack, self.chip, self.index = rack, chip, index


def dot(a, b, dims=NN):
    return lax.dot_general(a, b, dims, preferred_element_type=F32)


def split(x):
    hi = x.astype(BF16)
    lo = (x - hi.astype(F32)).astype(BF16)
    return hi, lo


def kernel(
    dims,
    points_h,
    counts_h,
    cells_h,
    pw_h,
    pfn_gain_h,
    pfn_bias_h,
    w4_h,
    bn_gain_h,
    bn_bias_h,
    cot_h,
    feat,
    out_g,
    norms,
    pgrad,
    points,
    counts,
    cells,
    pw,
    pw_s,
    pfn_gain,
    pfn_bias,
    w4,
    bn_gain,
    bn_bias,
    cot,
    xs,
    gs,
    hs,
    res,
    wn,
    wfs,
    wbs,
    wb0s,
    g4,
    onehot,
    par,
    cot_s,
    grads,
    bm,
    mx,
    sq,
    xh,
    yy,
    st0,
    st,
    rs,
    rbuf,
    rx,
    rxbuf,
    in_sem,
    st_send,
    st_recv,
    rs_send,
    rs_recv,
    rx_send,
    rx_recv,
    ag_send,
    ag_recv,
):
    n_rack, n_chip, sweeps, maxp, gh, gw, pill, ch, owners = dims
    n = n_rack * n_chip
    h2, w2 = gh // 2, gw // 2
    plane = h2 * w2
    pix = sweeps * plane
    ch3 = 3 * ch
    my_rack, my_chip = lax.axis_index("rack"), lax.axis_index("chip")
    me = my_rack * n_chip + my_chip

    fetches = [
        (points_h, points),
        (counts_h, counts),
        (cells_h, cells),
        (pw_h, pw),
        (pw_h, pw_s),
        (pfn_gain_h, pfn_gain),
        (pfn_bias_h, pfn_bias),
        (bn_gain_h, bn_gain),
        (bn_bias_h, bn_bias),
        (w4_h, w4),
        (cot_h, cot),
    ]
    fetches = [pltpu.make_async_copy(a, b, in_sem.at[i]) for i, (a, b) in enumerate(fetches)]

    def device(t):
        if isinstance(t, Peer):
            return {"rack": t.rack, "chip": t.chip}
        return {"rack": lax.div(t, n_chip), "chip": lax.rem(t, n_chip)}

    def far(k):
        dr, dc = divmod(k, n_chip)
        return -min(dc, n_chip - dc) - min(dr, n_rack - dr)

    def peers(body):
        if n <= 32:
            for k in sorted(range(1, n), key=far):
                dr, dc = divmod(k, n_chip)
                rack = lax.rem(my_rack + dr, n_rack) if dr else my_rack
                chip = lax.rem(my_chip + dc, n_chip) if dc else my_chip
                body(Peer(rack, chip, rack * n_chip + chip))
            return

        def step(k, carry):
            body(lax.rem(me + k, n))
            return carry

        lax.fori_loop(1, n, step, 0)

    for f in fetches:
        f.start()
    barrier = pltpu.get_barrier_semaphore()
    peers(
        lambda t: pl.semaphore_signal(
            barrier, inc=1, device_id=device(t), device_id_type=pl.DeviceIdType.MESH
        )
    )

    def remote(src, dst, send, recv, t):
        pltpu.make_async_remote_copy(
            src_ref=src,
            dst_ref=dst,
            send_sem=send,
            recv_sem=recv,
            device_id=device(t),
            device_id_type=pl.DeviceIdType.MESH,
        ).start()

    def landed(ref, sem):
        pltpu.make_async_copy(ref, ref, sem).wait()

    def send_row(buf, rnd, row):
        buf[rnd, me] = row
        mine = buf.at[rnd, me]
        peers(lambda t: remote(mine, mine, st_send.at[rnd], st_recv.at[rnd], t))

    def wait_row(buf, rnd):
        landed(buf.at[rnd, pl.ds(0, n - 1)], st_recv.at[rnd])
        return buf[rnd]

    def send_parts(src, dst, send, recv):
        def go(t):
            index = t.index if isinstance(t, Peer) else t

            def copy():
                remote(src.at[index], dst.at[me], send, recv, t)

            if owners == n:
                copy()
            else:
                pl.when(t.index < owners if isinstance(t, Peer) else t < owners)(copy)

        peers(go)

    def when_owner(body):
        if owners == n:
            body()
        else:
            pl.when(me < owners)(body)

    lane = lax.broadcasted_iota(jnp.int32, (1, 2 * ch), 1)

    def add_parts(layer):
        def body():
            landed(rbuf.at[layer, pl.ds(0, n - 1)], rs_recv.at[layer])
            rbuf[layer, me] = rs[layer, me]
            total = jnp.sum(rbuf[layer], axis=0)
            if layer in LINEAR:
                at = LINEAR.index(layer)
                landed(rxbuf.at[at, pl.ds(0, n - 1)], rx_recv.at[at])
                rxbuf[at, me] = rx[at, me]
                extra = jnp.sum(rxbuf[at], axis=0)

                def mine(row):
                    even = jnp.sum(jnp.where(lane == 2 * me, row, 0.0), axis=1, keepdims=True)
                    odd = jnp.sum(jnp.where(lane == 2 * me + 1, row, 0.0), axis=1, keepdims=True)
                    return jnp.where(lane < ch, even, odd)

                sums = sigmas[layer]
                inv = pltpu.roll(sq[layer, 0:1, :], ch, axis=1)
                gain = par[11 + layer : 12 + layer, :]
                c_dy = mine(sums / entries)
                c_dx = mine(pltpu.roll(sums, ch, axis=1) / entries)
                total = total - c_dy * extra[9:18] - c_dx * extra[0:9]
                total = mine(gain * inv) * total
            grads[layer, me] = total
            out = grads.at[layer, me]
            peers(lambda t: remote(out, out, ag_send.at[layer], ag_recv.at[layer], t))

        when_owner(body)

    for f in fetches[0:5]:
        f.wait()
    slot = lax.broadcasted_iota(jnp.int32, (maxp, pill), 0)
    per_sweep = []
    spots = []
    totals = [jnp.zeros((1, 1), F32)] * 9
    n_loc = jnp.zeros((1, 1), F32)
    for s in range(sweeps):
        valid = slot < counts[s : s + 1, :]
        mask = valid.astype(F32)
        cnt = counts[s : s + 1, :].astype(F32)
        sums = [jnp.sum(points[s, f] * mask, axis=0, keepdims=True) for f in range(4)]
        cents = [sums[f] / cnt for f in range(3)]
        cell = cells[s : s + 1, :]
        row = lax.shift_right_logical(cell, gw.bit_length() - 1)
        col = cell & (gw - 1)
        col_pos = col.astype(F32) * (2.0 / gw) - 1.0
        row_pos = row.astype(F32) * (2.0 / gh) - 1.0
        feats = sums + [sums[f] - cnt * cents[f] for f in range(3)]
        feats += [sums[0] - cnt * col_pos, sums[1] - cnt * row_pos]
        totals = [t + jnp.sum(f, axis=1, keepdims=True) for t, f in zip(totals, feats)]
        n_loc = n_loc + jnp.sum(cnt, axis=1, keepdims=True)
        per_sweep.append(cents + [col_pos, row_pos])
        spot = ((row & 1) * 2 + (col & 1)) * plane
        spot = spot + lax.shift_right_logical(row, 1) * w2 + lax.shift_right_logical(col, 1)
        spots.append(spot)
    for f in fetches[5:9]:
        f.wait()
    par[...] = jnp.zeros(par.shape, F32)
    par[0:9, 0:ch] = pw[...]
    par[9:10, 0:ch] = pfn_gain[...]
    par[10:11, 0:ch] = pfn_bias[...]
    par[11 : 11 + LAYERS, 0:ch] = bn_gain[...]
    par[11 + LAYERS : 11 + 2 * LAYERS, 0:ch] = bn_bias[...]
    par_cols = par[...].T
    pw_cols = par_cols[0:ch, 0:9]
    gain_c, bias_c = par_cols[0:ch, 9:10], par_cols[0:ch, 10:11]
    bn_cols = par_cols[0:ch, 11 : 11 + 2 * LAYERS]
    m_loc = jnp.zeros((ch, 1), F32)
    for f in range(9):
        m_loc = m_loc + pw_cols[:, f : f + 1] * totals[f]
    m_loc = m_loc / n_loc
    for s in range(sweeps):
        base = -m_loc
        for f in range(5):
            base = base - pw_cols[:, f + 4 : f + 5] * per_sweep[s][f]
        bm[s] = base

    def one_channel(c, carry):
        wx = pw_s[0, c] + pw_s[4, c] + pw_s[7, c]
        wy = pw_s[1, c] + pw_s[5, c] + pw_s[8, c]
        wz = pw_s[2, c] + pw_s[6, c]
        wr = pw_s[3, c]
        total = jnp.zeros((8, pill), F32)
        for s in range(sweeps):
            most = jnp.full((8, pill), LOWEST, F32)
            shift_by = bm[s, pl.ds(c, 1), :]
            have = counts[s : s + 1, :]
            for k in range(maxp // 8):
                part = pl.ds(8 * k, 8)
                ids = lax.broadcasted_iota(jnp.int32, (8, pill), 0) + 8 * k
                ok = ids < have
                h = points[s, 0, part, :] * wx + points[s, 1, part, :] * wy
                h = h + points[s, 2, part, :] * wz + points[s, 3, part, :] * wr + shift_by
                most = jnp.maximum(most, jnp.where(ok, h, LOWEST))
                h = jnp.where(ok, h, 0.0)
                total = total + h * h
            mx[s, c] = most
        folded = total[:, 0:128]
        for t in range(1, pill // 128):
            folded = folded + total[:, t * 128 : (t + 1) * 128]
        sq[c] = folded
        return carry

    lax.fori_loop(0, ch, one_channel, 0)
    both = jnp.concatenate([jnp.broadcast_to(m_loc, (ch, 128)), jnp.sum(sq[...], axis=1)], axis=0)
    turned = both.T
    row = jnp.where(lane < ch, turned[0:1, :], jnp.sum(turned, axis=0, keepdims=True))
    row = jnp.concatenate([row, jnp.broadcast_to(n_loc, (1, 2 * ch))], axis=1)

    pl.semaphore_wait(barrier, n - 1)
    send_row(st0, 0, row)

    col = lax.broadcasted_iota(jnp.int32, (1, w2), 1)
    tiles = pix // w2

    def tile(x, t):
        return x[:, t * w2 : (t + 1) * w2]

    def shift(x, d):
        if d == 0:
            return x
        ok = col >= -d if d < 0 else col < w2 - d
        return jnp.concatenate(
            [jnp.where(ok, pltpu.roll(tile(x, t), (-d) % w2, axis=1), 0.0) for t in range(tiles)],
            axis=1,
        )

    def down(x, d):
        parts = []
        for s in range(sweeps):
            for r in range(h2):
                inside = 0 <= r + d < h2
                t = s * h2 + r + d
                parts.append(tile(x, t) if inside else jnp.zeros((x.shape[0], w2), x.dtype))
        return jnp.concatenate(parts, axis=1)

    def stack_rows(at, per_tap):
        for a, (x, d) in enumerate(per_tap):
            for h in range(2):
                xs[at, h, a * ch : (a + 1) * ch, :] = down(x[h], d) if d else x[h]

    def stack_cols(ref, step, x):
        for b in range(3):
            for h, part in enumerate(split(shift(x, 1 - b))):
                ref[h * step + b * ch : h * step + (b + 1) * ch, :] = part

    def natural(layer):
        half = ch // 2
        for b in range(3):
            v = [w4[3 * a + b, :, layer, :] for a in range(3)]
            for k in range(2):
                v3 = [x[:, k * ch : (k + 1) * ch] for x in v]
                rows = pl.ds(b * ch + k, half, stride=2)
                wn[0, rows, :] = jnp.concatenate(v3[0:2], axis=1)
                wn[1, rows, :] = jnp.concatenate([v3[2], v3[2]], axis=1)
        return jnp.concatenate([wn[0], wn[1, :, 0:ch]], axis=1)

    def weights(layer):
        w = natural(layer)
        hi, lo = split(w)
        if layer == 0:
            for h, part in enumerate((hi, lo)):
                wfs[0, h * 2 * ch : (h * 2 + 1) * ch, :] = part[0:ch]
                wfs[0, (h * 2 + 1) * ch : (h * 2 + 2) * ch, :] = part[2 * ch : ch3]
                wfs[0, (4 + h) * ch : (5 + h) * ch, :] = part[ch : 2 * ch]
            first_backward_weights(w.T)
        else:
            wfs[layer, 0:ch3, :] = hi
            wfs[layer, ch3 : 2 * ch3, :] = lo
            hi, lo = split(w.T)
            wbs[layer - 1, 0:ch3, :] = hi
            wbs[layer - 1, ch3 : 2 * ch3, :] = lo

    def first_backward_weights(w):
        zero = jnp.zeros((ch, ch), F32)
        tap_of = {(0, 0): 1, (1, 0): 2, (1, 1): 0}
        for k in range(4):
            line = []
            for j in range(4):
                a, b = tap_of.get((k // 2, j // 2)), tap_of.get((k % 2, j % 2))
                none = a is None or b is None
                line.append(zero if none else w[a * ch : (a + 1) * ch, b * ch : (b + 1) * ch])
            hi, lo = split(jnp.concatenate(line, axis=1))
            wb0s[k * ch : (k + 1) * ch, :] = hi
            wb0s[(4 + k) * ch : (5 + k) * ch, :] = lo

    for s in range(sweeps):
        for k in range(4):
            ids = lax.broadcasted_iota(jnp.int32, (plane, pill), 0) + k * plane
            onehot[s, k * plane : (k + 1) * plane, :] = (ids == spots[s]).astype(F32).astype(BF16)
    for s in range(sweeps):
        bm[s] = jnp.max(mx[s], axis=1)
    for f in fetches[9:11]:
        f.wait()
    weights(0)
    inside = lax.broadcasted_iota(jnp.int32, (16, pix), 0)
    cols = lax.broadcasted_iota(jnp.int32, (16, pix), 1) & (w2 - 1)
    ones = ((inside == 0) & (cols < w2 - 1)) | (inside == 1) | ((inside == 2) & (cols >= 1))
    hs[ch3 : ch3 + 16, :] = ones.astype(F32).astype(BF16)
    hs[2 * ch3 + 16 : 2 * ch3 + 32, :] = jnp.zeros((16, pix), BF16)

    def columns(row):
        turned = jnp.broadcast_to(row, (8, 2 * ch)).T
        return turned[0:ch, 0:1], turned[ch : 2 * ch, 0:1]

    got = wait_row(st0, 0)
    n_all = jnp.sum(got[:, :, 2 * ch :], axis=0)
    rows = got[:, :, 0 : 2 * ch]
    weighted = got[:, :, 2 * ch :]
    means = jnp.sum(rows * weighted, axis=0) / n_all
    dev = rows - means[None]
    spread = jnp.sum(dev * dev * weighted, axis=0)
    second = (jnp.sum(rows, axis=0) + pltpu.roll(spread, ch, axis=1)) / n_all
    mean_c, inv_c = columns(jnp.where(lane < ch, means, lax.rsqrt(second + EPS)))
    scale_c = gain_c * inv_c
    shift_c = scale_c * (m_loc - mean_c) + bias_c

    planes = [[], [], [], []]
    for s in range(sweeps):
        pillar = jnp.maximum(bm[s] * scale_c + shift_c, 0.0)
        hi, lo = split(pillar)
        placed = dot(jnp.concatenate([hi, lo], axis=0), onehot[s], NT)
        for k in range(4):
            part = placed[:, k * plane : (k + 1) * plane]
            planes[k].append(part[0:ch] + part[ch : 2 * ch])
    planes = [split(jnp.concatenate(p, axis=1)) for p in planes]
    for k in range(2):
        stack_rows(k, [(planes[2 + k], -1), (planes[k], 0), (planes[2 + k], 0)])

    entries_loc = float(pix)
    entries = float(pix * n)

    def fold(x):
        out = x[:, 0:128]
        for t in range(1, pix // 128):
            out = out + x[:, t * 128 : (t + 1) * 128]
        return out

    def parts3(w, k, at):
        big = dot(w, xs[at, 0])
        return big[0:k] + big[k : 2 * k] + dot(w[0:k], xs[at, 1])

    def convolve(layer):
        if layer == 0:
            y = parts3(wfs[0, 0 : 4 * ch, :], 2 * ch, 1)
            return parts3(wfs[0, 4 * ch : 6 * ch, :], ch, 0) + y[ch : 2 * ch] + shift(y[0:ch], -1)
        y = parts3(wfs[layer], ch3, layer + 1)
        return y[ch : 2 * ch] + shift(y[0:ch], -1) + shift(y[2 * ch : ch3], 1)

    def correlate(both, k, at):
        big = dot(both, xs[at, 0], NT)
        return big[0:k] + big[k : 2 * k] + dot(both[0:k], xs[at, 1], NT)

    def pairs(store):
        half = ch // 2
        for b in range(3):
            for a in range(3):
                at = slice((a % 2) * ch, (a % 2 + 1) * ch)
                even = res[a // 2, pl.ds(b * ch, half, stride=2), :]
                odd = res[a // 2, pl.ds(b * ch + 1, half, stride=2), :]
                store(3 * a + b, jnp.concatenate([even[:, at], odd[:, at]], axis=1))

    def keep(at, x):
        res[0, at, :] = x[:, 0 : 2 * ch]
        res[1, at, 0:ch] = x[:, 2 * ch : ch3]

    def send_grad(ref, layer):
        if layer == 0:
            some = jnp.concatenate([ref[0 : 2 * ch, :], ref[ch3 : ch3 + 2 * ch, :]], axis=0)
            odd = correlate(some, 2 * ch, 1)
            some = jnp.concatenate([ref[ch : 2 * ch, :], ref[ch3 + ch : ch3 + 2 * ch, :]], axis=0)
            keep(slice(0, ch), odd[0:ch])
            keep(slice(ch, 2 * ch), correlate(some, ch, 0))
            keep(slice(2 * ch, ch3), odd[ch : 2 * ch])
        else:
            keep(slice(0, ch3), correlate(ref[...], ch3, layer + 1))

        def store(t, line):
            rs[layer, :, t, :] = line

        pairs(store)
        send_parts(rs.at[layer], rbuf.at[layer], rs_send.at[layer], rs_recv.at[layer])

    def send_extra(layer):
        at = LINEAR.index(layer)
        k = ch3 + 16
        stack_cols(hs, k, xh[layer])
        if layer == 0:
            even, odd = correlate(hs[...], k, 0), correlate(hs[...], k, 1)
            keep(slice(0, ch), odd[0:ch])
            keep(slice(ch, 2 * ch), even[ch : 2 * ch])
            keep(slice(2 * ch, ch3), odd[ch : 2 * ch])
            window = [odd[ch3 : ch3 + 1], even[ch3 + 1 : ch3 + 2], odd[ch3 + 1 : ch3 + 2]]
        else:
            both = correlate(hs[...], k, layer + 1)
            keep(slice(0, ch3), both[0:ch3])
            window = [both[ch3 + b : ch3 + b + 1] for b in range(3)]

        def store(t, line):
            rx[at, :, t, :] = line

        pairs(store)
        for b in range(3):
            for a in range(3):
                one = window[b][:, a * ch : (a + 1) * ch]
                line = jnp.concatenate([one, one], axis=1)
                rx[at, :, 9 + 3 * a + b, :] = jnp.broadcast_to(line, (owners, 2 * ch))
        send_parts(rx.at[at], rxbuf.at[at], rx_send.at[at], rx_recv.at[at])

    def finish(layer):
        scale, off, inv, by = affine[layer]
        d = xh[layer]
        y = scale * d + off
        xh[layer] = inv * (d - by)
        sig = jax.nn.sigmoid(y)
        yy[layer] = sig * (1.0 + y * (1.0 - sig))

    affine = []
    sigmas = {}
    act = None
    for layer in range(LAYERS):
        z = convolve(layer)
        sums = fold(z)
        m_loc = jnp.sum(sums, axis=1, keepdims=True) / entries_loc
        d = z - m_loc
        turned = jnp.concatenate([sums, fold(d * d)], axis=0).T
        row = jnp.sum(turned, axis=0, keepdims=True)
        row = jnp.where(lane < ch, row / entries_loc, row)
        send_row(st, layer + 1, row)
        xh[layer] = d
        if layer + 1 < LAYERS:
            weights(layer + 1)
        else:
            for s in range(sweeps):
                for r in range(h2):
                    at = s * plane + r * w2
                    cot_s[:, at : at + w2] = cot[s, :, r, :]
        if layer > 0:
            finish(layer - 1)
            if layer - 1 in LINEAR:
                send_extra(layer - 1)
        rows = wait_row(st, layer + 1)
        total = jnp.sum(rows, axis=0)
        means = total / float(n)
        dev = rows - means[None]
        spread = jnp.sum(dev * dev, axis=0) * entries_loc
        second = (total + pltpu.roll(spread, ch, axis=1)) / entries
        row = jnp.where(lane < ch, means, lax.rsqrt(second + EPS))
        mean_c, inv_c = columns(row)
        sq[layer, :, :] = jnp.broadcast_to(row, (8, 2 * ch))
        by = mean_c - m_loc
        scale = bn_cols[:, layer : layer + 1] * inv_c
        off = bn_cols[:, LAYERS + layer : LAYERS + layer + 1] - scale * by
        affine.append((scale, off, inv_c, by))
        y = scale * xh[layer] + off
        act = y * jax.nn.sigmoid(y)
        if layer + 1 < LAYERS:
            hi_lo = split(act)
            stack_rows(layer + 2, [(hi_lo, -1), (hi_lo, 0), (hi_lo, 1)])
        else:
            finish(layer)

    def backward(layer):
        w = wbs[layer - 1]
        big = dot(w, gs[0:ch3, :])
        v = big[0:ch3] + big[ch3 : 2 * ch3] + dot(w[0:ch3], gs[ch3 : 2 * ch3, :])
        return v[ch : 2 * ch] + down(v[0:ch], 1) + down(v[2 * ch : ch3], -1)

    u = cot_s[...]
    for layer in range(LAYERS - 1, -1, -1):
        gy = u * yy[layer]
        turned = jnp.concatenate([fold(gy), fold(gy * xh[layer])], axis=0).T
        rnd = 2 * LAYERS - layer
        send_row(st, rnd, jnp.sum(turned, axis=0, keepdims=True))
        if layer == LAYERS - 1:
            for s in range(sweeps):
                for r in range(h2):
                    at = s * plane + r * w2
                    feat[s, :, r, :] = act[:, at : at + w2]
        if layer in LINEAR:
            stack_cols(hs, ch3, gy)
            send_grad(hs.at[0 : 2 * ch3, :], layer)
        if layer + 1 < LAYERS and layer + 1 not in LINEAR:
            send_grad(gs, layer + 1)
        for done in range(layer + 1, LAYERS):
            if done == layer + (1 if done in LINEAR else 2):
                add_parts(done)
        row = jnp.sum(wait_row(st, rnd), axis=0)
        sigmas[layer] = row
        norms[0, layer : layer + 1, :] = row[:, ch : 2 * ch]
        norms[1, layer : layer + 1, :] = row[:, 0:ch]
        dy_c, dyx_c = columns(row / entries)
        gz = affine[layer][0] * (gy - dy_c - xh[layer] * dyx_c)
        if layer > 0:
            stack_cols(gs, ch3, gz)
            u = backward(layer)
    for dr in range(2):
        for dc in range(2):
            hi, lo = split(shift(down(gz, dr), dc))
            at = pl.ds((2 * dr + dc) * ch, ch)
            g4[0, at, :] = hi
            g4[1, at, :] = lo
    big = dot(wb0s[...], g4[0])
    u0 = big[0 : 4 * ch] + big[4 * ch :] + dot(wb0s[0 : 4 * ch, :], g4[1])
    for s in range(sweeps):
        total = None
        for k in range(4):
            hi, lo = split(u0[k * ch : (k + 1) * ch, s * plane : (s + 1) * plane])
            part = dot(
                jnp.concatenate([hi, lo], axis=0), onehot[s, k * plane : (k + 1) * plane, :]
            )
            total = part if total is None else total + part
        pgrad[s] = total[0:ch] + total[ch : 2 * ch]
    add_parts(0)

    def by_role(mine, theirs):
        if owners == n:
            mine()
        else:
            pl.when(me < owners)(mine)
            pl.when(me >= owners)(theirs)

    for layer in range(LAYERS - 1, -1, -1):
        others = grads.at[layer, pl.ds(0, owners - 1)]
        by_role(
            lambda: landed(others, ag_recv.at[layer]),
            lambda: landed(grads.at[layer], ag_recv.at[layer]),
        )
        for t in range(9):
            out_g[t, :, layer, :] = grads[layer, :, t, :]

    for rnd in range(2 * LAYERS + 1):
        landed((st0.at[0] if rnd == 0 else st.at[rnd]).at[pl.ds(0, n - 1)], st_send.at[rnd])
    for layer in range(LAYERS):
        by_role(
            lambda: landed(rs.at[layer, pl.ds(0, owners - 1)], rs_send.at[layer]),
            lambda: landed(rs.at[layer], rs_send.at[layer]),
        )
        when_owner(lambda: landed(rbuf.at[layer, pl.ds(0, n - 1)], ag_send.at[layer]))
    for at in range(len(LINEAR)):
        by_role(
            lambda: landed(rx.at[at, pl.ds(0, owners - 1)], rx_send.at[at]),
            lambda: landed(rx.at[at], rx_send.at[at]),
        )


def write_out(a, b, c, d, a_h, b_h, c_h, d_h, sem):
    pairs = [(a, a_h), (b, b_h), (c, c_h), (d, d_h)]
    copies = [pltpu.make_async_copy(x, y, sem.at[i]) for i, (x, y) in enumerate(pairs)]
    for x in copies:
        x.start()
    for x in copies:
        x.wait()


def per_device(
    n_rack,
    n_chip,
    points,
    counts,
    cells,
    pfn_weight,
    pfn_gain,
    pfn_bias,
    conv_weight,
    bn_gain,
    bn_bias,
    cotangent,
):
    sweeps, _, maxp, pill = points.shape
    ch = pfn_weight.shape[1]
    h2, w2 = cotangent.shape[2:]
    gh, gw = 2 * h2, 2 * w2
    n = n_rack * n_chip
    owners = ch // 2
    assert n >= owners and w2 == 128 and 2 * ch == 128
    pix = sweeps * h2 * w2
    ch3 = 3 * ch
    dims = (n_rack, n_chip, sweeps, maxp, gh, gw, pill, ch, owners)
    hbm = pl.BlockSpec(memory_space=pl.ANY)
    vmem = pl.BlockSpec(memory_space=pltpu.VMEM)
    extra = len(LINEAR)
    w4 = conv_weight.reshape(LAYERS, 9, owners, 2 * ch).transpose(1, 2, 0, 3)
    dma = pltpu.SemaphoreType.DMA
    outs = pl.pallas_call(
        functools.partial(kernel, dims),
        out_shape=(
            pltpu.VMEM((sweeps, ch, h2, w2), F32),
            pltpu.VMEM((9, owners, LAYERS, 2 * ch), F32),
            pltpu.VMEM((2, LAYERS, ch), F32),
            pltpu.VMEM((sweeps, ch, pill), F32),
        ),
        in_specs=[hbm] * 10,
        out_specs=(vmem,) * 4,
        scratch_shapes=[
            pltpu.VMEM((sweeps, 4, maxp, pill), F32),
            pltpu.VMEM((sweeps, pill), jnp.int32),
            pltpu.VMEM((sweeps, pill), jnp.int32),
            pltpu.VMEM((9, ch), F32),
            pltpu.SMEM((9, ch), F32),
            pltpu.VMEM((1, ch), F32),
            pltpu.VMEM((1, ch), F32),
            pltpu.VMEM((9, owners, LAYERS, 2 * ch), F32),
            pltpu.VMEM((LAYERS, ch), F32),
            pltpu.VMEM((LAYERS, ch), F32),
            pltpu.VMEM((sweeps, ch, h2, w2), F32),
            pltpu.VMEM((LAYERS + 1, 2, ch3, pix), BF16),
            pltpu.VMEM((2 * ch3, pix), BF16),
            pltpu.VMEM((2 * ch3 + 32, pix), BF16),
            pltpu.VMEM((2, ch3, 2 * ch), F32),
            pltpu.VMEM((2, ch3, 2 * ch), F32),
            pltpu.VMEM((LAYERS, 2 * ch3, ch3), BF16),
            pltpu.VMEM((LAYERS - 1, 2 * ch3, ch3), BF16),
            pltpu.VMEM((8 * ch, 4 * ch), BF16),
            pltpu.VMEM((2, 4 * ch, pix), BF16),
            pltpu.VMEM((sweeps, gh * gw, pill), BF16),
            pltpu.VMEM((32, 128), F32),
            pltpu.VMEM((ch, pix), F32),
            pltpu.VMEM((LAYERS, owners, 9, 2 * ch), F32),
            pltpu.VMEM((sweeps, ch, pill), F32),
            pltpu.VMEM((sweeps, ch, 8, pill), F32),
            pltpu.VMEM((ch, 8, 128), F32),
            pltpu.VMEM((LAYERS, ch, pix), F32),
            pltpu.VMEM((LAYERS, ch, pix), F32),
            pltpu.VMEM((1, n, 1, 4 * ch), F32),
            pltpu.VMEM((2 * LAYERS + 1, n, 1, 2 * ch), F32),
            pltpu.VMEM((LAYERS, owners, 9, 2 * ch), F32),
            pltpu.VMEM((LAYERS, n, 9, 2 * ch), F32),
            pltpu.VMEM((extra, owners, 18, 2 * ch), F32),
            pltpu.VMEM((extra, n, 18, 2 * ch), F32),
            dma((11,)),
            dma((2 * LAYERS + 1,)),
            dma((2 * LAYERS + 1,)),
            dma((LAYERS,)),
            dma((LAYERS,)),
            dma((extra,)),
            dma((extra,)),
            dma((LAYERS,)),
            dma((LAYERS,)),
        ],
        compiler_params=pltpu.CompilerParams(
            collective_id=0, has_side_effects=True, vmem_limit_bytes=56 * 1024 * 1024
        ),
    )(
        points,
        counts,
        cells,
        pfn_weight,
        pfn_gain.reshape(1, ch),
        pfn_bias.reshape(1, ch),
        w4,
        bn_gain,
        bn_bias,
        cotangent,
    )
    feat, out_g, norms, pgrad = pl.pallas_call(
        write_out,
        out_shape=tuple(jax.ShapeDtypeStruct(x.shape, x.dtype) for x in outs),
        in_specs=[vmem] * 4,
        out_specs=(hbm,) * 4,
        scratch_shapes=[dma((4,))],
    )(*[pltpu.with_memory_space_constraint(x, pltpu.VMEM) for x in outs])
    grads = out_g.transpose(2, 0, 1, 3).reshape(LAYERS, 9, ch * ch)
    return (feat, grads, norms, pgrad)


def solution(mesh):
    both = ("rack", "chip")
    return jax.shard_map(
        functools.partial(per_device, mesh.shape["rack"], mesh.shape["chip"]),
        mesh=mesh,
        in_specs=(
            P(both, None, None, None),
            P(both, None),
            P(both, None),
            P(),
            P(),
            P(),
            P(),
            P(),
            P(),
            P(both, None, None, None),
        ),
        out_specs=(
            P(both, None, None, None),
            P(),
            P(),
            P(both, None, None),
        ),
        check_vma=False,
    )
```

```python
import functools

import jax
import jax.numpy as jnp
from jax import lax
from jax.experimental import pallas as pl
from jax.experimental.pallas import tpu as pltpu
from jax.sharding import PartitionSpec as P

LAYERS = 4
LINEAR = (0, 1)
EPS = 1e-05
F32 = jnp.float32
BF16 = jnp.bfloat16
NN = (((1,), (0,)), ((), ()))
NT = (((1,), (1,)), ((), ()))
LOWEST = -3e38


class Peer:
    def __init__(self, rack, chip, index):
        self.rack, self.chip, self.index = rack, chip, index


def dot(a, b, dims=NN):
    return lax.dot_general(a, b, dims, preferred_element_type=F32)


def split(x):
    hi = x.astype(BF16)
    lo = (x - hi.astype(F32)).astype(BF16)
    return hi, lo


def kernel(
    dims,
    points_h,
    counts_h,
    cells_h,
    pw_h,
    pfn_gain_h,
    pfn_bias_h,
    w4_h,
    bn_gain_h,
    bn_bias_h,
    cot_h,
    feat,
    out_g,
    norms,
    pgrad,
    points,
    counts,
    cells,
    pw,
    pw_s,
    pfn_gain,
    pfn_bias,
    w4,
    bn_gain,
    bn_bias,
    cot,
    xs,
    gs,
    hs,
    res,
    wn,
    wfs,
    wbs,
    wb0s,
    g4,
    onehot,
    par,
    cot_s,
    grads,
    bm,
    mx,
    sq,
    xh,
    yy,
    st0,
    st,
    rs,
    ra,
    rp,
    rbuf,
    rx,
    rxa,
    rxp,
    rxbuf,
    in_sem,
    st_send,
    st_recv,
    ra_send,
    ra_recv,
    rs_send,
    rs_recv,
    rxa_send,
    rxa_recv,
    rx_send,
    rx_recv,
    ag_send,
    ag_recv,
    sh_send,
    sh_recv,
):
    n_rack, n_chip, sweeps, maxp, gh, gw, pill, ch, owners = dims
    n = n_rack * n_chip
    h2, w2 = gh // 2, gw // 2
    plane = h2 * w2
    pix = sweeps * plane
    ch3 = 3 * ch
    my_rack, my_chip = lax.axis_index("rack"), lax.axis_index("chip")
    me = my_rack * n_chip + my_chip
    half, n_same = owners // 2, n // 2
    core, my_x = lax.rem(my_rack, 2), lax.div(my_rack, 2)
    place = my_x * n_chip + my_chip
    slot_of_me = core * half + place
    twin = Peer(my_rack + 1 - 2 * core, my_chip, 0)

    fetches = [
        (points_h, points),
        (counts_h, counts),
        (cells_h, cells),
        (pw_h, pw),
        (pw_h, pw_s),
        (pfn_gain_h, pfn_gain),
        (pfn_bias_h, pfn_bias),
        (bn_gain_h, bn_gain),
        (bn_bias_h, bn_bias),
        (w4_h, w4),
        (cot_h, cot),
    ]
    fetches = [pltpu.make_async_copy(a, b, in_sem.at[i]) for i, (a, b) in enumerate(fetches)]

    def device(t):
        if isinstance(t, Peer):
            return {"rack": t.rack, "chip": t.chip}
        return {"rack": lax.div(t, n_chip), "chip": lax.rem(t, n_chip)}

    def far(k):
        dr, dc = divmod(k, n_chip)
        return -min(dc, n_chip - dc) - min(dr, n_rack - dr)

    def peers(body):
        if n <= 32:
            for k in sorted(range(1, n), key=far):
                dr, dc = divmod(k, n_chip)
                rack = lax.rem(my_rack + dr, n_rack) if dr else my_rack
                chip = lax.rem(my_chip + dc, n_chip) if dc else my_chip
                body(Peer(rack, chip, rack * n_chip + chip))
            return

        def step(k, carry):
            body(lax.rem(me + k, n))
            return carry

        lax.fori_loop(1, n, step, 0)

    for f in fetches:
        f.start()
    barrier = pltpu.get_barrier_semaphore()
    peers(
        lambda t: pl.semaphore_signal(
            barrier, inc=1, device_id=device(t), device_id_type=pl.DeviceIdType.MESH
        )
    )

    def remote(src, dst, send, recv, t):
        pltpu.make_async_remote_copy(
            src_ref=src,
            dst_ref=dst,
            send_sem=send,
            recv_sem=recv,
            device_id=device(t),
            device_id_type=pl.DeviceIdType.MESH,
        ).start()

    def landed(ref, sem):
        pltpu.make_async_copy(ref, ref, sem).wait()

    def send_row(buf, rnd, row):
        buf[rnd, me] = row
        mine = buf.at[rnd, me]
        peers(lambda t: remote(mine, mine, st_send.at[rnd], st_recv.at[rnd], t))

    def wait_row(buf, rnd):
        landed(buf.at[rnd, pl.ds(0, n - 1)], st_recv.at[rnd])
        return buf[rnd]

    def same_core(body):
        if n <= 32:
            for k in sorted(range(1, n_same), key=far):
                dx, dc = divmod(k, n_chip)
                x = lax.rem(my_x + dx, n_rack // 2) if dx else my_x
                chip = lax.rem(my_chip + dc, n_chip) if dc else my_chip
                body(Peer(x * 2 + core, chip, x * n_chip + chip))
            return

        def step(k, carry):
            at = lax.rem(place + k, n_same)
            body(Peer(lax.div(at, n_chip) * 2 + core, lax.rem(at, n_chip), at))
            return carry

        lax.fori_loop(1, n_same, step, 0)

    def to_twin(src, dst, send, recv):
        remote(src.at[pl.ds((1 - core) * half, half)], dst, send, recv, twin)

    def send_parts(src, came, both, dst, came_sem, send, recv):
        landed(came, came_sem)
        both[...] = src[pl.ds(core * half, half)] + came[...]

        def go(t):
            def copy():
                remote(both.at[t.index], dst.at[place], send, recv, t)

            if half == n_same:
                copy()
            else:
                pl.when(t.index < half)(copy)

        same_core(go)

    def pass_on(layer):
        send_parts(
            rs.at[layer],
            ra.at[layer],
            rp.at[layer],
            rbuf.at[layer],
            ra_recv.at[layer],
            rs_send.at[layer],
            rs_recv.at[layer],
        )

    def when_owner(body):
        if half == n_same:
            body()
        else:
            pl.when(place < half)(body)

    def by_role(mine, theirs):
        if half == n_same:
            mine()
        else:
            pl.when(place < half)(mine)
            pl.when(place >= half)(theirs)

    lane = lax.broadcasted_iota(jnp.int32, (1, 2 * ch), 1)

    def add_parts(layer):
        def body():
            landed(rbuf.at[layer, pl.ds(0, n_same - 1)], rs_recv.at[layer])
            rbuf[layer, place] = rp[layer, place]
            total = jnp.sum(rbuf[layer], axis=0)
            if layer in LINEAR:
                at = LINEAR.index(layer)
                landed(rxbuf.at[at, pl.ds(0, n_same - 1)], rx_recv.at[at])
                rxbuf[at, place] = rxp[at, place]
                extra = jnp.sum(rxbuf[at], axis=0)

                def mine(row):
                    even = jnp.sum(jnp.where(lane == 2 * slot_of_me, row, 0.0), axis=1, keepdims=True)
                    odd = jnp.sum(jnp.where(lane == 2 * slot_of_me + 1, row, 0.0), axis=1, keepdims=True)
                    return jnp.where(lane < ch, even, odd)

                sums = sigmas[layer]
                inv = pltpu.roll(sq[layer, 0:1, :], ch, axis=1)
                gain = par[11 + layer : 12 + layer, :]
                c_dy = mine(sums / entries)
                c_dx = mine(pltpu.roll(sums, ch, axis=1) / entries)
                total = total - c_dy * extra[9:18] - c_dx * extra[0:9]
                total = mine(gain * inv) * total
            grads[layer, slot_of_me] = total
            out = grads.at[layer, slot_of_me]
            same_core(lambda t: remote(out, out, ag_send.at[layer], ag_recv.at[layer], t))

        when_owner(body)

    def share(layer):
        by_role(
            lambda: landed(grads.at[layer, pl.ds(0, half - 1)], ag_recv.at[layer]),
            lambda: landed(grads.at[layer, pl.ds(0, half)], ag_recv.at[layer]),
        )
        ours = grads.at[layer, pl.ds(core * half, half)]
        remote(ours, ours, sh_send.at[layer], sh_recv.at[layer], twin)

    for f in fetches[0:5]:
        f.wait()
    slot = lax.broadcasted_iota(jnp.int32, (maxp, pill), 0)
    per_sweep = []
    spots = []
    totals = [jnp.zeros((1, 1), F32)] * 9
    n_loc = jnp.zeros((1, 1), F32)
    for s in range(sweeps):
        valid = slot < counts[s : s + 1, :]
        mask = valid.astype(F32)
        cnt = counts[s : s + 1, :].astype(F32)
        sums = [jnp.sum(points[s, f] * mask, axis=0, keepdims=True) for f in range(4)]
        cents = [sums[f] / cnt for f in range(3)]
        cell = cells[s : s + 1, :]
        row = lax.shift_right_logical(cell, gw.bit_length() - 1)
        col = cell & (gw - 1)
        col_pos = col.astype(F32) * (2.0 / gw) - 1.0
        row_pos = row.astype(F32) * (2.0 / gh) - 1.0
        feats = sums + [sums[f] - cnt * cents[f] for f in range(3)]
        feats += [sums[0] - cnt * col_pos, sums[1] - cnt * row_pos]
        totals = [t + jnp.sum(f, axis=1, keepdims=True) for t, f in zip(totals, feats)]
        n_loc = n_loc + jnp.sum(cnt, axis=1, keepdims=True)
        per_sweep.append(cents + [col_pos, row_pos])
        spot = ((row & 1) * 2 + (col & 1)) * plane
        spot = spot + lax.shift_right_logical(row, 1) * w2 + lax.shift_right_logical(col, 1)
        spots.append(spot)
    for f in fetches[5:9]:
        f.wait()
    par[...] = jnp.zeros(par.shape, F32)
    par[0:9, 0:ch] = pw[...]
    par[9:10, 0:ch] = pfn_gain[...]
    par[10:11, 0:ch] = pfn_bias[...]
    par[11 : 11 + LAYERS, 0:ch] = bn_gain[...]
    par[11 + LAYERS : 11 + 2 * LAYERS, 0:ch] = bn_bias[...]
    par_cols = par[...].T
    pw_cols = par_cols[0:ch, 0:9]
    gain_c, bias_c = par_cols[0:ch, 9:10], par_cols[0:ch, 10:11]
    bn_cols = par_cols[0:ch, 11 : 11 + 2 * LAYERS]
    m_loc = jnp.zeros((ch, 1), F32)
    for f in range(9):
        m_loc = m_loc + pw_cols[:, f : f + 1] * totals[f]
    m_loc = m_loc / n_loc
    for s in range(sweeps):
        base = -m_loc
        for f in range(5):
            base = base - pw_cols[:, f + 4 : f + 5] * per_sweep[s][f]
        bm[s] = base

    def one_channel(c, carry):
        wx = pw_s[0, c] + pw_s[4, c] + pw_s[7, c]
        wy = pw_s[1, c] + pw_s[5, c] + pw_s[8, c]
        wz = pw_s[2, c] + pw_s[6, c]
        wr = pw_s[3, c]
        total = jnp.zeros((8, pill), F32)
        for s in range(sweeps):
            most = jnp.full((8, pill), LOWEST, F32)
            shift_by = bm[s, pl.ds(c, 1), :]
            have = counts[s : s + 1, :]
            for k in range(maxp // 8):
                part = pl.ds(8 * k, 8)
                ids = lax.broadcasted_iota(jnp.int32, (8, pill), 0) + 8 * k
                ok = ids < have
                h = points[s, 0, part, :] * wx + points[s, 1, part, :] * wy
                h = h + points[s, 2, part, :] * wz + points[s, 3, part, :] * wr + shift_by
                most = jnp.maximum(most, jnp.where(ok, h, LOWEST))
                h = jnp.where(ok, h, 0.0)
                total = total + h * h
            mx[s, c] = most
        folded = total[:, 0:128]
        for t in range(1, pill // 128):
            folded = folded + total[:, t * 128 : (t + 1) * 128]
        sq[c] = folded
        return carry

    lax.fori_loop(0, ch, one_channel, 0)
    both = jnp.concatenate([jnp.broadcast_to(m_loc, (ch, 128)), jnp.sum(sq[...], axis=1)], axis=0)
    turned = both.T
    row = jnp.where(lane < ch, turned[0:1, :], jnp.sum(turned, axis=0, keepdims=True))
    row = jnp.concatenate([row, jnp.broadcast_to(n_loc, (1, 2 * ch))], axis=1)

    pl.semaphore_wait(barrier, n - 1)
    send_row(st0, 0, row)

    col = lax.broadcasted_iota(jnp.int32, (1, w2), 1)
    tiles = pix // w2

    def tile(x, t):
        return x[:, t * w2 : (t + 1) * w2]

    def shift(x, d):
        if d == 0:
            return x
        ok = col >= -d if d < 0 else col < w2 - d
        return jnp.concatenate(
            [jnp.where(ok, pltpu.roll(tile(x, t), (-d) % w2, axis=1), 0.0) for t in range(tiles)],
            axis=1,
        )

    def down(x, d):
        parts = []
        for s in range(sweeps):
            for r in range(h2):
                inside = 0 <= r + d < h2
                t = s * h2 + r + d
                parts.append(tile(x, t) if inside else jnp.zeros((x.shape[0], w2), x.dtype))
        return jnp.concatenate(parts, axis=1)

    def stack_rows(at, per_tap):
        for a, (x, d) in enumerate(per_tap):
            for h in range(2):
                xs[at, h, a * ch : (a + 1) * ch, :] = down(x[h], d) if d else x[h]

    def stack_cols(ref, step, x):
        for b in range(3):
            for h, part in enumerate(split(shift(x, 1 - b))):
                ref[h * step + b * ch : h * step + (b + 1) * ch, :] = part

    def natural(layer):
        half = ch // 2
        for b in range(3):
            v = [w4[3 * a + b, :, layer, :] for a in range(3)]
            for k in range(2):
                v3 = [x[:, k * ch : (k + 1) * ch] for x in v]
                rows = pl.ds(b * ch + k, half, stride=2)
                wn[0, rows, :] = jnp.concatenate(v3[0:2], axis=1)
                wn[1, rows, :] = jnp.concatenate([v3[2], v3[2]], axis=1)
        return jnp.concatenate([wn[0], wn[1, :, 0:ch]], axis=1)

    def weights(layer):
        w = natural(layer)
        hi, lo = split(w)
        if layer == 0:
            for h, part in enumerate((hi, lo)):
                wfs[0, h * 2 * ch : (h * 2 + 1) * ch, :] = part[0:ch]
                wfs[0, (h * 2 + 1) * ch : (h * 2 + 2) * ch, :] = part[2 * ch : ch3]
                wfs[0, (4 + h) * ch : (5 + h) * ch, :] = part[ch : 2 * ch]
            first_backward_weights(w.T)
        else:
            wfs[layer, 0:ch3, :] = hi
            wfs[layer, ch3 : 2 * ch3, :] = lo
            hi, lo = split(w.T)
            wbs[layer - 1, 0:ch3, :] = hi
            wbs[layer - 1, ch3 : 2 * ch3, :] = lo

    def first_backward_weights(w):
        zero = jnp.zeros((ch, ch), F32)
        tap_of = {(0, 0): 1, (1, 0): 2, (1, 1): 0}
        for k in range(4):
            line = []
            for j in range(4):
                a, b = tap_of.get((k // 2, j // 2)), tap_of.get((k % 2, j % 2))
                none = a is None or b is None
                line.append(zero if none else w[a * ch : (a + 1) * ch, b * ch : (b + 1) * ch])
            hi, lo = split(jnp.concatenate(line, axis=1))
            wb0s[k * ch : (k + 1) * ch, :] = hi
            wb0s[(4 + k) * ch : (5 + k) * ch, :] = lo

    for s in range(sweeps):
        for k in range(4):
            ids = lax.broadcasted_iota(jnp.int32, (plane, pill), 0) + k * plane
            onehot[s, k * plane : (k + 1) * plane, :] = (ids == spots[s]).astype(F32).astype(BF16)
    for s in range(sweeps):
        bm[s] = jnp.max(mx[s], axis=1)
    for f in fetches[9:11]:
        f.wait()
    weights(0)
    inside = lax.broadcasted_iota(jnp.int32, (16, pix), 0)
    cols = lax.broadcasted_iota(jnp.int32, (16, pix), 1) & (w2 - 1)
    ones = ((inside == 0) & (cols < w2 - 1)) | (inside == 1) | ((inside == 2) & (cols >= 1))
    hs[ch3 : ch3 + 16, :] = ones.astype(F32).astype(BF16)
    hs[2 * ch3 + 16 : 2 * ch3 + 32, :] = jnp.zeros((16, pix), BF16)

    def columns(row):
        turned = jnp.broadcast_to(row, (8, 2 * ch)).T
        return turned[0:ch, 0:1], turned[ch : 2 * ch, 0:1]

    got = wait_row(st0, 0)
    n_all = jnp.sum(got[:, :, 2 * ch :], axis=0)
    rows = got[:, :, 0 : 2 * ch]
    weighted = got[:, :, 2 * ch :]
    means = jnp.sum(rows * weighted, axis=0) / n_all
    dev = rows - means[None]
    spread = jnp.sum(dev * dev * weighted, axis=0)
    second = (jnp.sum(rows, axis=0) + pltpu.roll(spread, ch, axis=1)) / n_all
    mean_c, inv_c = columns(jnp.where(lane < ch, means, lax.rsqrt(second + EPS)))
    scale_c = gain_c * inv_c
    shift_c = scale_c * (m_loc - mean_c) + bias_c

    planes = [[], [], [], []]
    for s in range(sweeps):
        pillar = jnp.maximum(bm[s] * scale_c + shift_c, 0.0)
        hi, lo = split(pillar)
        placed = dot(jnp.concatenate([hi, lo], axis=0), onehot[s], NT)
        for k in range(4):
            part = placed[:, k * plane : (k + 1) * plane]
            planes[k].append(part[0:ch] + part[ch : 2 * ch])
    planes = [split(jnp.concatenate(p, axis=1)) for p in planes]
    for k in range(2):
        stack_rows(k, [(planes[2 + k], -1), (planes[k], 0), (planes[2 + k], 0)])

    entries_loc = float(pix)
    entries = float(pix * n)

    def fold(x):
        out = x[:, 0:128]
        for t in range(1, pix // 128):
            out = out + x[:, t * 128 : (t + 1) * 128]
        return out

    def parts3(w, k, at):
        big = dot(w, xs[at, 0])
        return big[0:k] + big[k : 2 * k] + dot(w[0:k], xs[at, 1])

    def convolve(layer):
        if layer == 0:
            y = parts3(wfs[0, 0 : 4 * ch, :], 2 * ch, 1)
            return parts3(wfs[0, 4 * ch : 6 * ch, :], ch, 0) + y[ch : 2 * ch] + shift(y[0:ch], -1)
        y = parts3(wfs[layer], ch3, layer + 1)
        return y[ch : 2 * ch] + shift(y[0:ch], -1) + shift(y[2 * ch : ch3], 1)

    def correlate(both, k, at):
        big = dot(both, xs[at, 0], NT)
        return big[0:k] + big[k : 2 * k] + dot(both[0:k], xs[at, 1], NT)

    def pairs(store):
        half = ch // 2
        for b in range(3):
            for a in range(3):
                at = slice((a % 2) * ch, (a % 2 + 1) * ch)
                even = res[a // 2, pl.ds(b * ch, half, stride=2), :]
                odd = res[a // 2, pl.ds(b * ch + 1, half, stride=2), :]
                store(3 * a + b, jnp.concatenate([even[:, at], odd[:, at]], axis=1))

    def keep(at, x):
        res[0, at, :] = x[:, 0 : 2 * ch]
        res[1, at, 0:ch] = x[:, 2 * ch : ch3]

    def send_grad(ref, layer):
        if layer == 0:
            some = jnp.concatenate([ref[0 : 2 * ch, :], ref[ch3 : ch3 + 2 * ch, :]], axis=0)
            odd = correlate(some, 2 * ch, 1)
            some = jnp.concatenate([ref[ch : 2 * ch, :], ref[ch3 + ch : ch3 + 2 * ch, :]], axis=0)
            keep(slice(0, ch), odd[0:ch])
            keep(slice(ch, 2 * ch), correlate(some, ch, 0))
            keep(slice(2 * ch, ch3), odd[ch : 2 * ch])
        else:
            keep(slice(0, ch3), correlate(ref[...], ch3, layer + 1))

        def store(t, line):
            rs[layer, :, t, :] = line

        pairs(store)
        to_twin(rs.at[layer], ra.at[layer], ra_send.at[layer], ra_recv.at[layer])

    def send_extra(layer):
        at = LINEAR.index(layer)
        k = ch3 + 16
        stack_cols(hs, k, xh[layer])
        if layer == 0:
            even, odd = correlate(hs[...], k, 0), correlate(hs[...], k, 1)
            keep(slice(0, ch), odd[0:ch])
            keep(slice(ch, 2 * ch), even[ch : 2 * ch])
            keep(slice(2 * ch, ch3), odd[ch : 2 * ch])
            window = [odd[ch3 : ch3 + 1], even[ch3 + 1 : ch3 + 2], odd[ch3 + 1 : ch3 + 2]]
        else:
            both = correlate(hs[...], k, layer + 1)
            keep(slice(0, ch3), both[0:ch3])
            window = [both[ch3 + b : ch3 + b + 1] for b in range(3)]

        def store(t, line):
            rx[at, :, t, :] = line

        pairs(store)
        for b in range(3):
            for a in range(3):
                one = window[b][:, a * ch : (a + 1) * ch]
                line = jnp.concatenate([one, one], axis=1)
                rx[at, :, 9 + 3 * a + b, :] = jnp.broadcast_to(line, (owners, 2 * ch))
        to_twin(rx.at[at], rxa.at[at], rxa_send.at[at], rxa_recv.at[at])
        send_parts(
            rx.at[at],
            rxa.at[at],
            rxp.at[at],
            rxbuf.at[at],
            rxa_recv.at[at],
            rx_send.at[at],
            rx_recv.at[at],
        )

    def finish(layer):
        scale, off, inv, by = affine[layer]
        d = xh[layer]
        y = scale * d + off
        xh[layer] = inv * (d - by)
        sig = jax.nn.sigmoid(y)
        yy[layer] = sig * (1.0 + y * (1.0 - sig))

    affine = []
    sigmas = {}
    act = None
    for layer in range(LAYERS):
        z = convolve(layer)
        sums = fold(z)
        m_loc = jnp.sum(sums, axis=1, keepdims=True) / entries_loc
        d = z - m_loc
        turned = jnp.concatenate([sums, fold(d * d)], axis=0).T
        row = jnp.sum(turned, axis=0, keepdims=True)
        row = jnp.where(lane < ch, row / entries_loc, row)
        send_row(st, layer + 1, row)
        xh[layer] = d
        if layer + 1 < LAYERS:
            weights(layer + 1)
        else:
            for s in range(sweeps):
                for r in range(h2):
                    at = s * plane + r * w2
                    cot_s[:, at : at + w2] = cot[s, :, r, :]
        if layer > 0:
            finish(layer - 1)
            if layer - 1 in LINEAR:
                send_extra(layer - 1)
        rows = wait_row(st, layer + 1)
        total = jnp.sum(rows, axis=0)
        means = total / float(n)
        dev = rows - means[None]
        spread = jnp.sum(dev * dev, axis=0) * entries_loc
        second = (total + pltpu.roll(spread, ch, axis=1)) / entries
        row = jnp.where(lane < ch, means, lax.rsqrt(second + EPS))
        mean_c, inv_c = columns(row)
        sq[layer, :, :] = jnp.broadcast_to(row, (8, 2 * ch))
        by = mean_c - m_loc
        scale = bn_cols[:, layer : layer + 1] * inv_c
        off = bn_cols[:, LAYERS + layer : LAYERS + layer + 1] - scale * by
        affine.append((scale, off, inv_c, by))
        y = scale * xh[layer] + off
        act = y * jax.nn.sigmoid(y)
        if layer + 1 < LAYERS:
            hi_lo = split(act)
            stack_rows(layer + 2, [(hi_lo, -1), (hi_lo, 0), (hi_lo, 1)])
        else:
            finish(layer)

    def backward(layer):
        w = wbs[layer - 1]
        big = dot(w, gs[0:ch3, :])
        v = big[0:ch3] + big[ch3 : 2 * ch3] + dot(w[0:ch3], gs[ch3 : 2 * ch3, :])
        return v[ch : 2 * ch] + down(v[0:ch], 1) + down(v[2 * ch : ch3], -1)

    u = cot_s[...]
    for layer in range(LAYERS - 1, -1, -1):
        gy = u * yy[layer]
        turned = jnp.concatenate([fold(gy), fold(gy * xh[layer])], axis=0).T
        rnd = 2 * LAYERS - layer
        send_row(st, rnd, jnp.sum(turned, axis=0, keepdims=True))
        if layer == LAYERS - 1:
            for s in range(sweeps):
                for r in range(h2):
                    at = s * plane + r * w2
                    feat[s, :, r, :] = act[:, at : at + w2]
        if layer in LINEAR:
            stack_cols(hs, ch3, gy)
            send_grad(hs.at[0 : 2 * ch3, :], layer)
        if layer + 1 < LAYERS and layer + 1 not in LINEAR:
            send_grad(gs, layer + 1)
        if layer in LINEAR:
            pass_on(layer)
        if layer + 1 < LAYERS and layer + 1 not in LINEAR:
            pass_on(layer + 1)
        for done in range(LAYERS - 1, layer, -1):
            if done == layer + (1 if done in LINEAR else 2):
                add_parts(done)
        if layer == 0:
            share(LAYERS - 1)
        row = jnp.sum(wait_row(st, rnd), axis=0)
        sigmas[layer] = row
        norms[0, layer : layer + 1, :] = row[:, ch : 2 * ch]
        norms[1, layer : layer + 1, :] = row[:, 0:ch]
        dy_c, dyx_c = columns(row / entries)
        gz = affine[layer][0] * (gy - dy_c - xh[layer] * dyx_c)
        if layer > 0:
            stack_cols(gs, ch3, gz)
            u = backward(layer)
    for dr in range(2):
        for dc in range(2):
            hi, lo = split(shift(down(gz, dr), dc))
            at = pl.ds((2 * dr + dc) * ch, ch)
            g4[0, at, :] = hi
            g4[1, at, :] = lo
    big = dot(wb0s[...], g4[0])
    u0 = big[0 : 4 * ch] + big[4 * ch :] + dot(wb0s[0 : 4 * ch, :], g4[1])
    for s in range(sweeps):
        total = None
        for k in range(4):
            hi, lo = split(u0[k * ch : (k + 1) * ch, s * plane : (s + 1) * plane])
            part = dot(
                jnp.concatenate([hi, lo], axis=0), onehot[s, k * plane : (k + 1) * plane, :]
            )
            total = part if total is None else total + part
        pgrad[s] = total[0:ch] + total[ch : 2 * ch]
    add_parts(0)

    for layer in range(LAYERS - 2, -1, -1):
        share(layer)

    for layer in range(LAYERS - 1, -1, -1):
        landed(grads.at[layer, pl.ds(0, half)], sh_recv.at[layer])
        for t in range(9):
            out_g[t, :, layer, :] = grads[layer, :, t, :]

    for rnd in range(2 * LAYERS + 1):
        landed((st0.at[0] if rnd == 0 else st.at[rnd]).at[pl.ds(0, n - 1)], st_send.at[rnd])
    for layer in range(LAYERS):
        landed(ra.at[layer], ra_send.at[layer])
        landed(grads.at[layer, pl.ds(0, half)], sh_send.at[layer])
        by_role(
            lambda: landed(rp.at[layer, pl.ds(0, half - 1)], rs_send.at[layer]),
            lambda: landed(rp.at[layer], rs_send.at[layer]),
        )
        when_owner(lambda: landed(rbuf.at[layer, pl.ds(0, n_same - 1)], ag_send.at[layer]))
    for at in range(len(LINEAR)):
        landed(rxa.at[at], rxa_send.at[at])
        by_role(
            lambda: landed(rxp.at[at, pl.ds(0, half - 1)], rx_send.at[at]),
            lambda: landed(rxp.at[at], rx_send.at[at]),
        )


def write_out(a, b, c, d, a_h, b_h, c_h, d_h, sem):
    pairs = [(a, a_h), (b, b_h), (c, c_h), (d, d_h)]
    copies = [pltpu.make_async_copy(x, y, sem.at[i]) for i, (x, y) in enumerate(pairs)]
    for x in copies:
        x.start()
    for x in copies:
        x.wait()


def per_device(
    n_rack,
    n_chip,
    points,
    counts,
    cells,
    pfn_weight,
    pfn_gain,
    pfn_bias,
    conv_weight,
    bn_gain,
    bn_bias,
    cotangent,
):
    sweeps, _, maxp, pill = points.shape
    ch = pfn_weight.shape[1]
    h2, w2 = cotangent.shape[2:]
    gh, gw = 2 * h2, 2 * w2
    n = n_rack * n_chip
    owners = ch // 2
    assert n >= owners and n_rack % 2 == 0 and w2 == 128 and 2 * ch == 128
    pix = sweeps * h2 * w2
    ch3 = 3 * ch
    dims = (n_rack, n_chip, sweeps, maxp, gh, gw, pill, ch, owners)
    hbm = pl.BlockSpec(memory_space=pl.ANY)
    vmem = pl.BlockSpec(memory_space=pltpu.VMEM)
    extra = len(LINEAR)
    w4 = conv_weight.reshape(LAYERS, 9, owners, 2 * ch).transpose(1, 2, 0, 3)
    dma = pltpu.SemaphoreType.DMA
    outs = pl.pallas_call(
        functools.partial(kernel, dims),
        out_shape=(
            pltpu.VMEM((sweeps, ch, h2, w2), F32),
            pltpu.VMEM((9, owners, LAYERS, 2 * ch), F32),
            pltpu.VMEM((2, LAYERS, ch), F32),
            pltpu.VMEM((sweeps, ch, pill), F32),
        ),
        in_specs=[hbm] * 10,
        out_specs=(vmem,) * 4,
        scratch_shapes=[
            pltpu.VMEM((sweeps, 4, maxp, pill), F32),
            pltpu.VMEM((sweeps, pill), jnp.int32),
            pltpu.VMEM((sweeps, pill), jnp.int32),
            pltpu.VMEM((9, ch), F32),
            pltpu.SMEM((9, ch), F32),
            pltpu.VMEM((1, ch), F32),
            pltpu.VMEM((1, ch), F32),
            pltpu.VMEM((9, owners, LAYERS, 2 * ch), F32),
            pltpu.VMEM((LAYERS, ch), F32),
            pltpu.VMEM((LAYERS, ch), F32),
            pltpu.VMEM((sweeps, ch, h2, w2), F32),
            pltpu.VMEM((LAYERS + 1, 2, ch3, pix), BF16),
            pltpu.VMEM((2 * ch3, pix), BF16),
            pltpu.VMEM((2 * ch3 + 32, pix), BF16),
            pltpu.VMEM((2, ch3, 2 * ch), F32),
            pltpu.VMEM((2, ch3, 2 * ch), F32),
            pltpu.VMEM((LAYERS, 2 * ch3, ch3), BF16),
            pltpu.VMEM((LAYERS - 1, 2 * ch3, ch3), BF16),
            pltpu.VMEM((8 * ch, 4 * ch), BF16),
            pltpu.VMEM((2, 4 * ch, pix), BF16),
            pltpu.VMEM((sweeps, gh * gw, pill), BF16),
            pltpu.VMEM((32, 128), F32),
            pltpu.VMEM((ch, pix), F32),
            pltpu.VMEM((LAYERS, owners, 9, 2 * ch), F32),
            pltpu.VMEM((sweeps, ch, pill), F32),
            pltpu.VMEM((sweeps, ch, 8, pill), F32),
            pltpu.VMEM((ch, 8, 128), F32),
            pltpu.VMEM((LAYERS, ch, pix), F32),
            pltpu.VMEM((LAYERS, ch, pix), F32),
            pltpu.VMEM((1, n, 1, 4 * ch), F32),
            pltpu.VMEM((2 * LAYERS + 1, n, 1, 2 * ch), F32),
            pltpu.VMEM((LAYERS, owners, 9, 2 * ch), F32),
            pltpu.VMEM((LAYERS, owners // 2, 9, 2 * ch), F32),
            pltpu.VMEM((LAYERS, owners // 2, 9, 2 * ch), F32),
            pltpu.VMEM((LAYERS, n // 2, 9, 2 * ch), F32),
            pltpu.VMEM((extra, owners, 18, 2 * ch), F32),
            pltpu.VMEM((extra, owners // 2, 18, 2 * ch), F32),
            pltpu.VMEM((extra, owners // 2, 18, 2 * ch), F32),
            pltpu.VMEM((extra, n // 2, 18, 2 * ch), F32),
            dma((11,)),
            dma((2 * LAYERS + 1,)),
            dma((2 * LAYERS + 1,)),
            dma((LAYERS,)),
            dma((LAYERS,)),
            dma((LAYERS,)),
            dma((LAYERS,)),
            dma((extra,)),
            dma((extra,)),
            dma((extra,)),
            dma((extra,)),
            dma((LAYERS,)),
            dma((LAYERS,)),
            dma((LAYERS,)),
            dma((LAYERS,)),
        ],
        compiler_params=pltpu.CompilerParams(
            collective_id=0, has_side_effects=True, vmem_limit_bytes=56 * 1024 * 1024
        ),
    )(
        points,
        counts,
        cells,
        pfn_weight,
        pfn_gain.reshape(1, ch),
        pfn_bias.reshape(1, ch),
        w4,
        bn_gain,
        bn_bias,
        cotangent,
    )
    feat, out_g, norms, pgrad = pl.pallas_call(
        write_out,
        out_shape=tuple(jax.ShapeDtypeStruct(x.shape, x.dtype) for x in outs),
        in_specs=[vmem] * 4,
        out_specs=(hbm,) * 4,
        scratch_shapes=[dma((4,))],
    )(*[pltpu.with_memory_space_constraint(x, pltpu.VMEM) for x in outs])
    grads = out_g.transpose(2, 0, 1, 3).reshape(LAYERS, 9, ch * ch)
    return (feat, grads, norms, pgrad)


def solution(mesh):
    both = ("rack", "chip")
    return jax.shard_map(
        functools.partial(per_device, mesh.shape["rack"], mesh.shape["chip"]),
        mesh=mesh,
        in_specs=(
            P(both, None, None, None),
            P(both, None),
            P(both, None),
            P(),
            P(),
            P(),
            P(),
            P(),
            P(),
            P(both, None, None, None),
        ),
        out_specs=(
            P(both, None, None, None),
            P(),
            P(),
            P(both, None, None),
        ),
        check_vma=False,
    )
```

```python
import functools

import jax
import jax.numpy as jnp
from jax import lax
from jax.experimental import pallas as pl
from jax.experimental.pallas import tpu as pltpu
from jax.sharding import PartitionSpec as P

LAYERS = 4
LINEAR = (0, 1)
EPS = 1e-05
F32 = jnp.float32
BF16 = jnp.bfloat16
NN = (((1,), (0,)), ((), ()))
NT = (((1,), (1,)), ((), ()))
LOWEST = -3e38


class Peer:
    def __init__(self, rack, chip, index):
        self.rack, self.chip, self.index = rack, chip, index


def dot(a, b, dims=NN):
    return lax.dot_general(a, b, dims, preferred_element_type=F32)


def split(x):
    hi = x.astype(BF16)
    lo = (x - hi.astype(F32)).astype(BF16)
    return hi, lo


def kernel(
    dims,
    points_h,
    counts_h,
    cells_h,
    pw_h,
    pfn_gain_h,
    pfn_bias_h,
    w4_h,
    bn_gain_h,
    bn_bias_h,
    cot_h,
    feat,
    out_g,
    norms,
    pgrad,
    points,
    counts,
    cells,
    pw,
    pw_s,
    pfn_gain,
    pfn_bias,
    w4,
    bn_gain,
    bn_bias,
    cot,
    xs,
    gs,
    hs,
    res,
    wn,
    wfs,
    wbs,
    wb0s,
    g4,
    onehot,
    par,
    cot_s,
    grads,
    bm,
    mx,
    sq,
    xh,
    yy,
    st0,
    st,
    rs,
    ra,
    rp,
    rbuf,
    rx,
    rxa,
    rxp,
    rxbuf,
    in_sem,
    st_send,
    st_recv,
    ra_send,
    ra_recv,
    rs_send,
    rs_recv,
    rxa_send,
    rxa_recv,
    rx_send,
    rx_recv,
    ag_send,
    ag_recv,
    sh_send,
    sh_recv,
):
    n_rack, n_chip, sweeps, maxp, gh, gw, pill, ch, owners = dims
    n = n_rack * n_chip
    h2, w2 = gh // 2, gw // 2
    plane = h2 * w2
    pix = sweeps * plane
    ch3 = 3 * ch
    my_rack, my_chip = lax.axis_index("rack"), lax.axis_index("chip")
    me = my_rack * n_chip + my_chip
    n_same = n // 2
    n_own = min(n_same, owners)
    per = owners // n_own
    core, my_x = lax.rem(my_rack, 2), lax.div(my_rack, 2)
    place = my_x * n_chip + my_chip
    twin = Peer(my_rack + 1 - 2 * core, my_chip, 0)

    fetches = [
        (points_h, points),
        (counts_h, counts),
        (cells_h, cells),
        (pw_h, pw),
        (pw_h, pw_s),
        (pfn_gain_h, pfn_gain),
        (pfn_bias_h, pfn_bias),
        (bn_gain_h, bn_gain),
        (bn_bias_h, bn_bias),
        (w4_h, w4),
        (cot_h, cot),
    ]
    fetches = [pltpu.make_async_copy(a, b, in_sem.at[i]) for i, (a, b) in enumerate(fetches)]

    def device(t):
        if isinstance(t, Peer):
            return {"rack": t.rack, "chip": t.chip}
        return {"rack": lax.div(t, n_chip), "chip": lax.rem(t, n_chip)}

    def flipped(x, size):
        out = []
        for m in range(size):
            y = x
            for bit in (1, 2, 4, 8, 16):
                if m & bit:
                    y = y + bit * (1 - 2 * lax.rem(lax.div(x, bit), 2))
            out.append(y)
        return out

    def is_power(k):
        return k & (k - 1) == 0

    few = n <= 32 and is_power(n_rack) and is_power(n_chip)
    if few:
        racks, chips = flipped(my_rack, n_rack), flipped(my_chip, n_chip)

    def far(k):
        r, c = divmod(k, n_chip)
        return -(c // 2 + c % 2 + r // 2 + 0.3 * (r % 2))

    def peers(body):
        if few:
            for k in sorted(range(1, n), key=far):
                r, c = divmod(k, n_chip)
                body(Peer(racks[r], chips[c], racks[r] * n_chip + chips[c]))
            return

        def step(k, carry):
            body(lax.rem(me + k, n))
            return carry

        lax.fori_loop(1, n, step, 0)

    for f in fetches:
        f.start()
    barrier = pltpu.get_barrier_semaphore()
    peers(
        lambda t: pl.semaphore_signal(
            barrier, inc=1, device_id=device(t), device_id_type=pl.DeviceIdType.MESH
        )
    )

    def remote(src, dst, send, recv, t):
        pltpu.make_async_remote_copy(
            src_ref=src,
            dst_ref=dst,
            send_sem=send,
            recv_sem=recv,
            device_id=device(t),
            device_id_type=pl.DeviceIdType.MESH,
        ).start()

    def landed(ref, sem):
        pltpu.make_async_copy(ref, ref, sem).wait()

    def send_row(buf, rnd, row):
        buf[rnd, me] = row
        mine = buf.at[rnd, me]
        peers(lambda t: remote(mine, mine, st_send.at[rnd], st_recv.at[rnd], t))

    def wait_row(buf, rnd):
        landed(buf.at[rnd, pl.ds(0, n - 1)], st_recv.at[rnd])
        return buf[rnd]

    def same_core(body):
        if few:
            for k in sorted(range(n), key=far):
                r, c = divmod(k, n_chip)
                if k > 0 and r % 2 == 0:
                    x = lax.div(racks[r], 2)
                    body(Peer(racks[r], chips[c], x * n_chip + chips[c]))
            return

        def step(k, carry):
            at = lax.rem(place + k, n_same)
            body(Peer(lax.div(at, n_chip) * 2 + core, lax.rem(at, n_chip), at))
            return carry

        lax.fori_loop(1, n_same, step, 0)

    def on_core(k, body):
        pl.when(core == k)(body)

    def to_twin(src, dst, send, recv):
        on_core(0, lambda: remote(src, dst, send, recv, twin))

    def when_owner(body):
        on_core(1, body if n_own == n_same else lambda: pl.when(place < n_own)(body))

    def by_role(mine, theirs):
        if n_own == n_same:
            mine()
        else:
            pl.when(place < n_own)(mine)
            pl.when(place >= n_own)(theirs)

    def send_parts(src, came, both, dst, came_sem, send, recv):
        def body():
            landed(came, came_sem)
            both[...] = src[...] + came[...]

            def go(t):
                def copy():
                    remote(both.at[t.index], dst.at[place], send, recv, t)

                if n_own == n_same:
                    copy()
                else:
                    pl.when(t.index < n_own)(copy)

            same_core(go)

        on_core(1, body)

    def pass_on(layer):
        send_parts(
            rs.at[layer],
            ra.at[layer],
            rp.at[layer],
            rbuf.at[layer],
            ra_recv.at[layer],
            rs_send.at[layer],
            rs_recv.at[layer],
        )

    lane = lax.broadcasted_iota(jnp.int32, (1, 2 * ch), 1)

    def add_parts(layer):
        def body():
            landed(rbuf.at[layer, pl.ds(0, n_same - 1)], rs_recv.at[layer])
            rbuf[layer, place] = rp[layer, place]
            total = jnp.sum(rbuf[layer], axis=0)
            if layer in LINEAR:
                at = LINEAR.index(layer)
                landed(rxbuf.at[at, pl.ds(0, n_same - 1)], rx_recv.at[at])
                rxbuf[at, place] = rxp[at, place]
                extra = jnp.sum(rxbuf[at], axis=0)

                def mine(row, k):
                    first = 2 * (k * n_own + place)
                    even = jnp.sum(jnp.where(lane == first, row, 0.0), axis=1, keepdims=True)
                    odd = jnp.sum(jnp.where(lane == first + 1, row, 0.0), axis=1, keepdims=True)
                    return jnp.where(lane < ch, even, odd)

                sums = sigmas[layer]
                inv = pltpu.roll(sq[layer, 0:1, :], ch, axis=1)
                gain = par[11 + layer : 12 + layer, :]
                window = extra[9 * per : 9 * per + 9]
                parts = []
                for k in range(per):
                    c_dy = mine(sums / entries, k)
                    c_dx = mine(pltpu.roll(sums, ch, axis=1) / entries, k)
                    at = slice(9 * k, 9 * k + 9)
                    part = total[at] - c_dy * window - c_dx * extra[at]
                    parts.append(mine(gain * inv, k) * part)
                for k in range(per):
                    grads[layer, place, 9 * k : 9 * k + 9, :] = parts[k]
            else:
                grads[layer, place] = total
            out = grads.at[layer, place]
            same_core(lambda t: remote(out, out, ag_send.at[layer], ag_recv.at[layer], t))

        when_owner(body)

    def share(layer):
        def body():
            by_role(
                lambda: landed(grads.at[layer, pl.ds(0, n_own - 1)], ag_recv.at[layer]),
                lambda: landed(grads.at[layer], ag_recv.at[layer]),
            )
            whole = grads.at[layer]
            remote(whole, whole, sh_send.at[layer], sh_recv.at[layer], twin)

        on_core(1, body)

    for f in fetches[0:5]:
        f.wait()
    slot = lax.broadcasted_iota(jnp.int32, (maxp, pill), 0)
    per_sweep = []
    spots = []
    totals = [jnp.zeros((1, 1), F32)] * 9
    n_loc = jnp.zeros((1, 1), F32)
    for s in range(sweeps):
        valid = slot < counts[s : s + 1, :]
        mask = valid.astype(F32)
        cnt = counts[s : s + 1, :].astype(F32)
        sums = [jnp.sum(points[s, f] * mask, axis=0, keepdims=True) for f in range(4)]
        cents = [sums[f] / cnt for f in range(3)]
        cell = cells[s : s + 1, :]
        row = lax.shift_right_logical(cell, gw.bit_length() - 1)
        col = cell & (gw - 1)
        col_pos = col.astype(F32) * (2.0 / gw) - 1.0
        row_pos = row.astype(F32) * (2.0 / gh) - 1.0
        feats = sums + [sums[f] - cnt * cents[f] for f in range(3)]
        feats += [sums[0] - cnt * col_pos, sums[1] - cnt * row_pos]
        totals = [t + jnp.sum(f, axis=1, keepdims=True) for t, f in zip(totals, feats)]
        n_loc = n_loc + jnp.sum(cnt, axis=1, keepdims=True)
        per_sweep.append(cents + [col_pos, row_pos])
        spot = ((row & 1) * 2 + (col & 1)) * plane
        spot = spot + lax.shift_right_logical(row, 1) * w2 + lax.shift_right_logical(col, 1)
        spots.append(spot)
    for f in fetches[5:9]:
        f.wait()
    par[...] = jnp.zeros(par.shape, F32)
    par[0:9, 0:ch] = pw[...]
    par[9:10, 0:ch] = pfn_gain[...]
    par[10:11, 0:ch] = pfn_bias[...]
    par[11 : 11 + LAYERS, 0:ch] = bn_gain[...]
    par[11 + LAYERS : 11 + 2 * LAYERS, 0:ch] = bn_bias[...]
    par_cols = par[...].T
    pw_cols = par_cols[0:ch, 0:9]
    gain_c, bias_c = par_cols[0:ch, 9:10], par_cols[0:ch, 10:11]
    bn_cols = par_cols[0:ch, 11 : 11 + 2 * LAYERS]
    m_loc = jnp.zeros((ch, 1), F32)
    for f in range(9):
        m_loc = m_loc + pw_cols[:, f : f + 1] * totals[f]
    m_loc = m_loc / n_loc
    for s in range(sweeps):
        base = -m_loc
        for f in range(5):
            base = base - pw_cols[:, f + 4 : f + 5] * per_sweep[s][f]
        bm[s] = base

    def one_channel(c, carry):
        wx = pw_s[0, c] + pw_s[4, c] + pw_s[7, c]
        wy = pw_s[1, c] + pw_s[5, c] + pw_s[8, c]
        wz = pw_s[2, c] + pw_s[6, c]
        wr = pw_s[3, c]
        total = jnp.zeros((8, pill), F32)
        for s in range(sweeps):
            most = jnp.full((8, pill), LOWEST, F32)
            shift_by = bm[s, pl.ds(c, 1), :]
            have = counts[s : s + 1, :]
            for k in range(maxp // 8):
                part = pl.ds(8 * k, 8)
                ids = lax.broadcasted_iota(jnp.int32, (8, pill), 0) + 8 * k
                ok = ids < have
                h = points[s, 0, part, :] * wx + points[s, 1, part, :] * wy
                h = h + points[s, 2, part, :] * wz + points[s, 3, part, :] * wr + shift_by
                most = jnp.maximum(most, jnp.where(ok, h, LOWEST))
                h = jnp.where(ok, h, 0.0)
                total = total + h * h
            mx[s, c] = most
        folded = total[:, 0:128]
        for t in range(1, pill // 128):
            folded = folded + total[:, t * 128 : (t + 1) * 128]
        sq[c] = folded
        return carry

    lax.fori_loop(0, ch, one_channel, 0)
    both = jnp.concatenate([jnp.broadcast_to(m_loc, (ch, 128)), jnp.sum(sq[...], axis=1)], axis=0)
    turned = both.T
    row = jnp.where(lane < ch, turned[0:1, :], jnp.sum(turned, axis=0, keepdims=True))
    row = jnp.concatenate([row, jnp.broadcast_to(n_loc, (1, 2 * ch))], axis=1)

    pl.semaphore_wait(barrier, n - 1)
    send_row(st0, 0, row)

    col = lax.broadcasted_iota(jnp.int32, (1, w2), 1)
    tiles = pix // w2

    def tile(x, t):
        return x[:, t * w2 : (t + 1) * w2]

    def shift(x, d):
        if d == 0:
            return x
        ok = col >= -d if d < 0 else col < w2 - d
        return jnp.concatenate(
            [jnp.where(ok, pltpu.roll(tile(x, t), (-d) % w2, axis=1), 0.0) for t in range(tiles)],
            axis=1,
        )

    def down(x, d):
        parts = []
        for s in range(sweeps):
            for r in range(h2):
                inside = 0 <= r + d < h2
                t = s * h2 + r + d
                parts.append(tile(x, t) if inside else jnp.zeros((x.shape[0], w2), x.dtype))
        return jnp.concatenate(parts, axis=1)

    def stack_rows(at, per_tap):
        for a, (x, d) in enumerate(per_tap):
            for h in range(2):
                xs[at, h, a * ch : (a + 1) * ch, :] = down(x[h], d) if d else x[h]

    def stack_cols(ref, step, x):
        for b in range(3):
            for h, part in enumerate(split(shift(x, 1 - b))):
                ref[h * step + b * ch : h * step + (b + 1) * ch, :] = part

    def natural(layer):
        half = ch // 2
        for b in range(3):
            v = [w4[3 * a + b, :, layer, :] for a in range(3)]
            for k in range(2):
                v3 = [x[:, k * ch : (k + 1) * ch] for x in v]
                rows = pl.ds(b * ch + k, half, stride=2)
                wn[0, rows, :] = jnp.concatenate(v3[0:2], axis=1)
                wn[1, rows, :] = jnp.concatenate([v3[2], v3[2]], axis=1)
        return jnp.concatenate([wn[0], wn[1, :, 0:ch]], axis=1)

    def weights(layer):
        w = natural(layer)
        hi, lo = split(w)
        if layer == 0:
            for h, part in enumerate((hi, lo)):
                wfs[0, h * 2 * ch : (h * 2 + 1) * ch, :] = part[0:ch]
                wfs[0, (h * 2 + 1) * ch : (h * 2 + 2) * ch, :] = part[2 * ch : ch3]
                wfs[0, (4 + h) * ch : (5 + h) * ch, :] = part[ch : 2 * ch]
            first_backward_weights(w.T)
        else:
            wfs[layer, 0:ch3, :] = hi
            wfs[layer, ch3 : 2 * ch3, :] = lo
            hi, lo = split(w.T)
            wbs[layer - 1, 0:ch3, :] = hi
            wbs[layer - 1, ch3 : 2 * ch3, :] = lo

    def first_backward_weights(w):
        zero = jnp.zeros((ch, ch), F32)
        tap_of = {(0, 0): 1, (1, 0): 2, (1, 1): 0}
        for k in range(4):
            line = []
            for j in range(4):
                a, b = tap_of.get((k // 2, j // 2)), tap_of.get((k % 2, j % 2))
                none = a is None or b is None
                line.append(zero if none else w[a * ch : (a + 1) * ch, b * ch : (b + 1) * ch])
            hi, lo = split(jnp.concatenate(line, axis=1))
            wb0s[k * ch : (k + 1) * ch, :] = hi
            wb0s[(4 + k) * ch : (5 + k) * ch, :] = lo

    for s in range(sweeps):
        spot = jnp.broadcast_to(spots[s].astype(F32), (8, pill)).T[:, 0:1]
        for k in range(4):
            ids = lax.broadcasted_iota(jnp.int32, (pill, plane), 1) + k * plane
            hit = ids.astype(F32) == spot
            onehot[s, :, k * plane : (k + 1) * plane] = hit.astype(F32).astype(BF16)
    for s in range(sweeps):
        bm[s] = jnp.max(mx[s], axis=1)
    for f in fetches[9:11]:
        f.wait()
    weights(0)
    inside = lax.broadcasted_iota(jnp.int32, (16, pix), 0)
    cols = lax.broadcasted_iota(jnp.int32, (16, pix), 1) & (w2 - 1)
    ones = ((inside == 0) & (cols < w2 - 1)) | (inside == 1) | ((inside == 2) & (cols >= 1))
    hs[ch3 : ch3 + 16, :] = ones.astype(F32).astype(BF16)
    hs[2 * ch3 + 16 : 2 * ch3 + 32, :] = jnp.zeros((16, pix), BF16)

    def columns(row):
        turned = jnp.broadcast_to(row, (8, 2 * ch)).T
        return turned[0:ch, 0:1], turned[ch : 2 * ch, 0:1]

    got = wait_row(st0, 0)
    n_all = jnp.sum(got[:, :, 2 * ch :], axis=0)
    rows = got[:, :, 0 : 2 * ch]
    weighted = got[:, :, 2 * ch :]
    means = jnp.sum(rows * weighted, axis=0) / n_all
    dev = rows - means[None]
    spread = jnp.sum(dev * dev * weighted, axis=0)
    second = (jnp.sum(rows, axis=0) + pltpu.roll(spread, ch, axis=1)) / n_all
    mean_c, inv_c = columns(jnp.where(lane < ch, means, lax.rsqrt(second + EPS)))
    scale_c = gain_c * inv_c
    shift_c = scale_c * (m_loc - mean_c) + bias_c

    planes = [[], [], [], []]
    for s in range(sweeps):
        pillar = jnp.maximum(bm[s] * scale_c + shift_c, 0.0)
        hi, lo = split(pillar)
        placed = dot(jnp.concatenate([hi, lo], axis=0), onehot[s])
        for k in range(4):
            part = placed[:, k * plane : (k + 1) * plane]
            planes[k].append(part[0:ch] + part[ch : 2 * ch])
    planes = [split(jnp.concatenate(p, axis=1)) for p in planes]
    for k in range(2):
        stack_rows(k, [(planes[2 + k], -1), (planes[k], 0), (planes[2 + k], 0)])

    entries_loc = float(pix)
    entries = float(pix * n)

    def fold(x):
        out = x[:, 0:128]
        for t in range(1, pix // 128):
            out = out + x[:, t * 128 : (t + 1) * 128]
        return out

    def parts3(w, k, at):
        big = dot(w, xs[at, 0])
        return big[0:k] + big[k : 2 * k] + dot(w[0:k], xs[at, 1])

    def convolve(layer):
        if layer == 0:
            y = parts3(wfs[0, 0 : 4 * ch, :], 2 * ch, 1)
            return parts3(wfs[0, 4 * ch : 6 * ch, :], ch, 0) + y[ch : 2 * ch] + shift(y[0:ch], -1)
        y = parts3(wfs[layer], ch3, layer + 1)
        return y[ch : 2 * ch] + shift(y[0:ch], -1) + shift(y[2 * ch : ch3], 1)

    def correlate(both, k, at):
        big = dot(both, xs[at, 0], NT)
        return big[0:k] + big[k : 2 * k] + dot(both[0:k], xs[at, 1], NT)

    def pairs(store):
        half = ch // 2
        for b in range(3):
            for a in range(3):
                at = slice((a % 2) * ch, (a % 2 + 1) * ch)
                even = res[a // 2, pl.ds(b * ch, half, stride=2), :]
                odd = res[a // 2, pl.ds(b * ch + 1, half, stride=2), :]
                store(3 * a + b, jnp.concatenate([even[:, at], odd[:, at]], axis=1))

    def keep(at, x):
        res[0, at, :] = x[:, 0 : 2 * ch]
        res[1, at, 0:ch] = x[:, 2 * ch : ch3]

    def send_grad(ref, layer):
        if layer == 0:
            some = jnp.concatenate([ref[0 : 2 * ch, :], ref[ch3 : ch3 + 2 * ch, :]], axis=0)
            odd = correlate(some, 2 * ch, 1)
            some = jnp.concatenate([ref[ch : 2 * ch, :], ref[ch3 + ch : ch3 + 2 * ch, :]], axis=0)
            keep(slice(0, ch), odd[0:ch])
            keep(slice(ch, 2 * ch), correlate(some, ch, 0))
            keep(slice(2 * ch, ch3), odd[ch : 2 * ch])
        else:
            keep(slice(0, ch3), correlate(ref[...], ch3, layer + 1))

        def store(t, line):
            for k in range(per):
                rs[layer, :, 9 * k + t, :] = line[k * n_own : (k + 1) * n_own]

        pairs(store)
        to_twin(rs.at[layer], ra.at[layer], ra_send.at[layer], ra_recv.at[layer])

    def send_extra(layer):
        at = LINEAR.index(layer)
        k = ch3 + 16
        stack_cols(hs, k, xh[layer])
        if layer == 0:
            even, odd = correlate(hs[...], k, 0), correlate(hs[...], k, 1)
            keep(slice(0, ch), odd[0:ch])
            keep(slice(ch, 2 * ch), even[ch : 2 * ch])
            keep(slice(2 * ch, ch3), odd[ch : 2 * ch])
            window = [odd[ch3 : ch3 + 1], even[ch3 + 1 : ch3 + 2], odd[ch3 + 1 : ch3 + 2]]
        else:
            both = correlate(hs[...], k, layer + 1)
            keep(slice(0, ch3), both[0:ch3])
            window = [both[ch3 + b : ch3 + b + 1] for b in range(3)]

        def store(t, line):
            for k in range(per):
                rx[at, :, 9 * k + t, :] = line[k * n_own : (k + 1) * n_own]

        pairs(store)
        for b in range(3):
            for a in range(3):
                one = window[b][:, a * ch : (a + 1) * ch]
                line = jnp.concatenate([one, one], axis=1)
                rx[at, :, 9 * per + 3 * a + b, :] = jnp.broadcast_to(line, (n_own, 2 * ch))
        to_twin(rx.at[at], rxa.at[at], rxa_send.at[at], rxa_recv.at[at])

    def pass_extra(layer):
        at = LINEAR.index(layer)
        send_parts(
            rx.at[at],
            rxa.at[at],
            rxp.at[at],
            rxbuf.at[at],
            rxa_recv.at[at],
            rx_send.at[at],
            rx_recv.at[at],
        )

    def finish(layer):
        scale, off, inv, by = affine[layer]
        d = xh[layer]
        y = scale * d + off
        xh[layer] = inv * (d - by)
        sig = jax.nn.sigmoid(y)
        yy[layer] = sig * (1.0 + y * (1.0 - sig))

    affine = []
    sigmas = {}
    act = None
    for layer in range(LAYERS):
        z = convolve(layer)
        sums = fold(z)
        m_loc = jnp.sum(sums, axis=1, keepdims=True) / entries_loc
        d = z - m_loc
        turned = jnp.concatenate([sums, fold(d * d)], axis=0).T
        row = jnp.sum(turned, axis=0, keepdims=True)
        row = jnp.where(lane < ch, row / entries_loc, row)
        send_row(st, layer + 1, row)
        xh[layer] = d
        if layer - 2 in LINEAR:
            pass_extra(layer - 2)
        if layer + 1 < LAYERS:
            weights(layer + 1)
        else:
            for s in range(sweeps):
                for r in range(h2):
                    at = s * plane + r * w2
                    cot_s[:, at : at + w2] = cot[s, :, r, :]
        if layer > 0:
            finish(layer - 1)
            if layer - 1 in LINEAR:
                send_extra(layer - 1)
        rows = wait_row(st, layer + 1)
        total = jnp.sum(rows, axis=0)
        means = total / float(n)
        dev = rows - means[None]
        spread = jnp.sum(dev * dev, axis=0) * entries_loc
        second = (total + pltpu.roll(spread, ch, axis=1)) / entries
        row = jnp.where(lane < ch, means, lax.rsqrt(second + EPS))
        mean_c, inv_c = columns(row)
        sq[layer, :, :] = jnp.broadcast_to(row, (8, 2 * ch))
        by = mean_c - m_loc
        scale = bn_cols[:, layer : layer + 1] * inv_c
        off = bn_cols[:, LAYERS + layer : LAYERS + layer + 1] - scale * by
        affine.append((scale, off, inv_c, by))
        y = scale * xh[layer] + off
        act = y * jax.nn.sigmoid(y)
        if layer + 1 < LAYERS:
            hi_lo = split(act)
            stack_rows(layer + 2, [(hi_lo, -1), (hi_lo, 0), (hi_lo, 1)])
        else:
            finish(layer)

    def backward(layer):
        w = wbs[layer - 1]
        big = dot(w, gs[0:ch3, :])
        v = big[0:ch3] + big[ch3 : 2 * ch3] + dot(w[0:ch3], gs[ch3 : 2 * ch3, :])
        return v[ch : 2 * ch] + down(v[0:ch], 1) + down(v[2 * ch : ch3], -1)

    u = cot_s[...]
    for layer in range(LAYERS - 1, -1, -1):
        gy = u * yy[layer]
        turned = jnp.concatenate([fold(gy), fold(gy * xh[layer])], axis=0).T
        rnd = 2 * LAYERS - layer
        send_row(st, rnd, jnp.sum(turned, axis=0, keepdims=True))
        if layer == LAYERS - 1:
            for s in range(sweeps):
                for r in range(h2):
                    at = s * plane + r * w2
                    feat[s, :, r, :] = act[:, at : at + w2]
        if layer in LINEAR:
            stack_cols(hs, ch3, gy)
            send_grad(hs.at[0 : 2 * ch3, :], layer)
        if layer + 1 < LAYERS and layer + 1 not in LINEAR:
            send_grad(gs, layer + 1)
        if layer in LINEAR:
            pass_on(layer)
        if layer == 0:
            share(LAYERS - 1)
        for done in range(LAYERS - 1, layer, -1):
            if done == layer + (1 if done in LINEAR else 2):
                add_parts(done)
        if layer + 1 < LAYERS and layer + 1 not in LINEAR:
            pass_on(layer + 1)
        row = jnp.sum(wait_row(st, rnd), axis=0)
        sigmas[layer] = row
        norms[0, layer : layer + 1, :] = row[:, ch : 2 * ch]
        norms[1, layer : layer + 1, :] = row[:, 0:ch]
        dy_c, dyx_c = columns(row / entries)
        gz = affine[layer][0] * (gy - dy_c - xh[layer] * dyx_c)
        if layer > 0:
            stack_cols(gs, ch3, gz)
            u = backward(layer)
    for dr in range(2):
        for dc in range(2):
            hi, lo = split(shift(down(gz, dr), dc))
            at = pl.ds((2 * dr + dc) * ch, ch)
            g4[0, at, :] = hi
            g4[1, at, :] = lo
    big = dot(wb0s[...], g4[0])
    u0 = big[0 : 4 * ch] + big[4 * ch :] + dot(wb0s[0 : 4 * ch, :], g4[1])
    for s in range(sweeps):
        total = None
        for k in range(4):
            hi, lo = split(u0[k * ch : (k + 1) * ch, s * plane : (s + 1) * plane])
            both = jnp.concatenate([hi, lo], axis=0)
            part = dot(both, onehot[s, :, k * plane : (k + 1) * plane], NT)
            total = part if total is None else total + part
        pgrad[s] = total[0:ch] + total[ch : 2 * ch]
    add_parts(0)

    def arrived(layer):
        on_core(0, lambda: landed(grads.at[layer], sh_recv.at[layer]))

    def unpack(layer):
        arrived(layer)
        for t in range(9):
            for k in range(per):
                part = grads[layer, :, 9 * k + t, :]
                out_g[t, k * n_own : (k + 1) * n_own, layer, :] = part

    def sent(ref, sem):
        by_role(lambda: landed(ref.at[pl.ds(0, n_own - 1)], sem), lambda: landed(ref, sem))

    def drain(layer):
        on_core(0, lambda: landed(ra.at[layer], ra_send.at[layer]))
        on_core(1, lambda: sent(rp.at[layer], rs_send.at[layer]))
        when_owner(lambda: landed(rbuf.at[layer, pl.ds(0, n_same - 1)], ag_send.at[layer]))

    for layer in range(LAYERS - 2, 0, -1):
        share(layer)
    for rnd in range(2 * LAYERS + 1):
        landed((st0.at[0] if rnd == 0 else st.at[rnd]).at[pl.ds(0, n - 1)], st_send.at[rnd])
    for at in range(len(LINEAR)):
        on_core(0, lambda: landed(rxa.at[at], rxa_send.at[at]))
        on_core(1, lambda: sent(rxp.at[at], rx_send.at[at]))
    for layer in range(LAYERS - 1, 0, -1):
        unpack(layer)
        drain(layer)
    share(0)
    drain(0)
    unpack(0)

    def shared():
        for layer in range(LAYERS):
            landed(grads.at[layer], sh_send.at[layer])

    on_core(1, shared)


def write_out(a, b, c, d, a_h, b_h, c_h, d_h, sem):
    pairs = [(a, a_h), (b, b_h), (c, c_h), (d, d_h)]
    copies = [pltpu.make_async_copy(x, y, sem.at[i]) for i, (x, y) in enumerate(pairs)]
    for x in copies:
        x.start()
    for x in copies:
        x.wait()


def per_device(
    n_rack,
    n_chip,
    points,
    counts,
    cells,
    pfn_weight,
    pfn_gain,
    pfn_bias,
    conv_weight,
    bn_gain,
    bn_bias,
    cotangent,
):
    sweeps, _, maxp, pill = points.shape
    ch = pfn_weight.shape[1]
    h2, w2 = cotangent.shape[2:]
    gh, gw = 2 * h2, 2 * w2
    n = n_rack * n_chip
    owners = ch // 2
    n_own = min(n // 2, owners)
    per = owners // n_own
    assert owners % n_own == 0 and n_rack % 2 == 0 and w2 == 128 and 2 * ch == 128
    pix = sweeps * h2 * w2
    ch3 = 3 * ch
    dims = (n_rack, n_chip, sweeps, maxp, gh, gw, pill, ch, owners)
    hbm = pl.BlockSpec(memory_space=pl.ANY)
    vmem = pl.BlockSpec(memory_space=pltpu.VMEM)
    extra = len(LINEAR)
    w4 = conv_weight.reshape(LAYERS, 9, owners, 2 * ch).transpose(1, 2, 0, 3)
    dma = pltpu.SemaphoreType.DMA
    outs = pl.pallas_call(
        functools.partial(kernel, dims),
        out_shape=(
            pltpu.VMEM((sweeps, ch, h2, w2), F32),
            pltpu.VMEM((9, owners, LAYERS, 2 * ch), F32),
            pltpu.VMEM((2, LAYERS, ch), F32),
            pltpu.VMEM((sweeps, ch, pill), F32),
        ),
        in_specs=[hbm] * 10,
        out_specs=(vmem,) * 4,
        scratch_shapes=[
            pltpu.VMEM((sweeps, 4, maxp, pill), F32),
            pltpu.VMEM((sweeps, pill), jnp.int32),
            pltpu.VMEM((sweeps, pill), jnp.int32),
            pltpu.VMEM((9, ch), F32),
            pltpu.SMEM((9, ch), F32),
            pltpu.VMEM((1, ch), F32),
            pltpu.VMEM((1, ch), F32),
            pltpu.VMEM((9, owners, LAYERS, 2 * ch), F32),
            pltpu.VMEM((LAYERS, ch), F32),
            pltpu.VMEM((LAYERS, ch), F32),
            pltpu.VMEM((sweeps, ch, h2, w2), F32),
            pltpu.VMEM((LAYERS + 1, 2, ch3, pix), BF16),
            pltpu.VMEM((2 * ch3, pix), BF16),
            pltpu.VMEM((2 * ch3 + 32, pix), BF16),
            pltpu.VMEM((2, ch3, 2 * ch), F32),
            pltpu.VMEM((2, ch3, 2 * ch), F32),
            pltpu.VMEM((LAYERS, 2 * ch3, ch3), BF16),
            pltpu.VMEM((LAYERS - 1, 2 * ch3, ch3), BF16),
            pltpu.VMEM((8 * ch, 4 * ch), BF16),
            pltpu.VMEM((2, 4 * ch, pix), BF16),
            pltpu.VMEM((sweeps, pill, gh * gw), BF16),
            pltpu.VMEM((32, 128), F32),
            pltpu.VMEM((ch, pix), F32),
            pltpu.VMEM((LAYERS, n_own, 9 * per, 2 * ch), F32),
            pltpu.VMEM((sweeps, ch, pill), F32),
            pltpu.VMEM((sweeps, ch, 8, pill), F32),
            pltpu.VMEM((ch, 8, 128), F32),
            pltpu.VMEM((LAYERS, ch, pix), F32),
            pltpu.VMEM((LAYERS, ch, pix), F32),
            pltpu.VMEM((1, n, 1, 4 * ch), F32),
            pltpu.VMEM((2 * LAYERS + 1, n, 1, 2 * ch), F32),
            pltpu.VMEM((LAYERS, n_own, 9 * per, 2 * ch), F32),
            pltpu.VMEM((LAYERS, n_own, 9 * per, 2 * ch), F32),
            pltpu.VMEM((LAYERS, n_own, 9 * per, 2 * ch), F32),
            pltpu.VMEM((LAYERS, n // 2, 9 * per, 2 * ch), F32),
            pltpu.VMEM((extra, n_own, 9 * per + 9, 2 * ch), F32),
            pltpu.VMEM((extra, n_own, 9 * per + 9, 2 * ch), F32),
            pltpu.VMEM((extra, n_own, 9 * per + 9, 2 * ch), F32),
            pltpu.VMEM((extra, n // 2, 9 * per + 9, 2 * ch), F32),
            dma((11,)),
            dma((2 * LAYERS + 1,)),
            dma((2 * LAYERS + 1,)),
            dma((LAYERS,)),
            dma((LAYERS,)),
            dma((LAYERS,)),
            dma((LAYERS,)),
            dma((extra,)),
            dma((extra,)),
            dma((extra,)),
            dma((extra,)),
            dma((LAYERS,)),
            dma((LAYERS,)),
            dma((LAYERS,)),
            dma((LAYERS,)),
        ],
        compiler_params=pltpu.CompilerParams(
            collective_id=0, has_side_effects=True, vmem_limit_bytes=56 * 1024 * 1024
        ),
    )(
        points,
        counts,
        cells,
        pfn_weight,
        pfn_gain.reshape(1, ch),
        pfn_bias.reshape(1, ch),
        w4,
        bn_gain,
        bn_bias,
        cotangent,
    )
    feat, out_g, norms, pgrad = pl.pallas_call(
        write_out,
        out_shape=tuple(jax.ShapeDtypeStruct(x.shape, x.dtype) for x in outs),
        in_specs=[vmem] * 4,
        out_specs=(hbm,) * 4,
        scratch_shapes=[dma((4,))],
    )(*[pltpu.with_memory_space_constraint(x, pltpu.VMEM) for x in outs])
    grads = out_g.transpose(2, 0, 1, 3).reshape(LAYERS, 9, ch * ch)
    return (feat, grads, norms, pgrad)


def solution(mesh):
    both = ("rack", "chip")
    return jax.shard_map(
        functools.partial(per_device, mesh.shape["rack"], mesh.shape["chip"]),
        mesh=mesh,
        in_specs=(
            P(both, None, None, None),
            P(both, None),
            P(both, None),
            P(),
            P(),
            P(),
            P(),
            P(),
            P(),
            P(both, None, None, None),
        ),
        out_specs=(
            P(both, None, None, None),
            P(),
            P(),
            P(both, None, None),
        ),
        check_vma=False,
    )
```

```python
import functools

import jax
import jax.numpy as jnp
from jax import lax
from jax.experimental import pallas as pl
from jax.experimental.pallas import tpu as pltpu
from jax.sharding import PartitionSpec as P

LAYERS = 4
LINEAR = (0, 1)
EPS = 1e-05
F32 = jnp.float32
BF16 = jnp.bfloat16
NN = (((1,), (0,)), ((), ()))
NT = (((1,), (1,)), ((), ()))
LOWEST = -3e38


class Peer:
    def __init__(self, rack, chip, index):
        self.rack, self.chip, self.index = rack, chip, index


def dot(a, b, dims=NN):
    return lax.dot_general(a, b, dims, preferred_element_type=F32)


def split(x):
    hi = x.astype(BF16)
    lo = (x - hi.astype(F32)).astype(BF16)
    return hi, lo


def kernel(
    dims,
    points_h,
    counts_h,
    cells_h,
    pw_h,
    pfn_gain_h,
    pfn_bias_h,
    w4_h,
    bn_gain_h,
    bn_bias_h,
    cot_h,
    feat,
    out_g,
    norms,
    pgrad,
    points,
    counts,
    cells,
    pw,
    pw_s,
    pfn_gain,
    pfn_bias,
    w4,
    bn_gain,
    bn_bias,
    cot,
    xs,
    gs,
    hs,
    res,
    wn,
    wfs,
    wbs,
    wb0s,
    g4,
    onehot,
    par,
    cot_s,
    grads,
    bm,
    mx,
    sq,
    xh,
    yy,
    st0,
    st,
    rs,
    ra,
    rp,
    rbuf,
    rx,
    rxa,
    rxp,
    rxbuf,
    in_sem,
    st_send,
    st_recv,
    ra_send,
    ra_recv,
    rs_send,
    rs_recv,
    rxa_send,
    rxa_recv,
    rx_send,
    rx_recv,
    ag_send,
    ag_recv,
    sh_send,
    sh_recv,
):
    n_rack, n_chip, sweeps, maxp, gh, gw, pill, ch, owners = dims
    n = n_rack * n_chip
    h2, w2 = gh // 2, gw // 2
    plane = h2 * w2
    pix = sweeps * plane
    ch3 = 3 * ch
    my_rack, my_chip = lax.axis_index("rack"), lax.axis_index("chip")
    me = my_rack * n_chip + my_chip
    n_same = n // 2
    n_own = min(n_same, owners)
    per = owners // n_own
    core, my_x = lax.rem(my_rack, 2), lax.div(my_rack, 2)
    place = my_x * n_chip + my_chip
    twin = Peer(my_rack + 1 - 2 * core, my_chip, 0)

    fetches = [
        (points_h, points),
        (counts_h, counts),
        (cells_h, cells),
        (pw_h, pw),
        (pw_h, pw_s),
        (pfn_gain_h, pfn_gain),
        (pfn_bias_h, pfn_bias),
        (bn_gain_h, bn_gain),
        (bn_bias_h, bn_bias),
        (w4_h, w4),
        (cot_h, cot),
    ]
    fetches = [pltpu.make_async_copy(a, b, in_sem.at[i]) for i, (a, b) in enumerate(fetches)]

    def device(t):
        if isinstance(t, Peer):
            return {"rack": t.rack, "chip": t.chip}
        return {"rack": lax.div(t, n_chip), "chip": lax.rem(t, n_chip)}

    def flipped(x, size):
        out = []
        for m in range(size):
            y = x
            for bit in (1, 2, 4, 8, 16):
                if m & bit:
                    y = y + bit * (1 - 2 * lax.rem(lax.div(x, bit), 2))
            out.append(y)
        return out

    def is_power(k):
        return k & (k - 1) == 0

    few = n <= 32 and is_power(n_rack) and is_power(n_chip)
    if few:
        racks, chips = flipped(my_rack, n_rack), flipped(my_chip, n_chip)

    def far(k):
        r, c = divmod(k, n_chip)
        return -(c // 2 + c % 2 + r // 2 + 0.3 * (r % 2))

    def peers(body):
        if few:
            for k in sorted(range(1, n), key=far):
                r, c = divmod(k, n_chip)
                body(Peer(racks[r], chips[c], racks[r] * n_chip + chips[c]))
            return

        def step(k, carry):
            body(lax.rem(me + k, n))
            return carry

        lax.fori_loop(1, n, step, 0)

    for f in fetches:
        f.start()
    barrier = pltpu.get_barrier_semaphore()
    peers(
        lambda t: pl.semaphore_signal(
            barrier, inc=1, device_id=device(t), device_id_type=pl.DeviceIdType.MESH
        )
    )

    def remote(src, dst, send, recv, t):
        pltpu.make_async_remote_copy(
            src_ref=src,
            dst_ref=dst,
            send_sem=send,
            recv_sem=recv,
            device_id=device(t),
            device_id_type=pl.DeviceIdType.MESH,
        ).start()

    def landed(ref, sem):
        pltpu.make_async_copy(ref, ref, sem).wait()

    def send_row(buf, rnd, row):
        buf[rnd, me] = row
        mine = buf.at[rnd, me]
        peers(lambda t: remote(mine, mine, st_send.at[rnd], st_recv.at[rnd], t))

    def wait_row(buf, rnd):
        landed(buf.at[rnd, pl.ds(0, n - 1)], st_recv.at[rnd])
        return buf[rnd]

    def same_core(body):
        if few:
            for k in sorted(range(n), key=far):
                r, c = divmod(k, n_chip)
                if k > 0 and r % 2 == 0:
                    x = lax.div(racks[r], 2)
                    body(Peer(racks[r], chips[c], x * n_chip + chips[c]))
            return

        def step(k, carry):
            at = lax.rem(place + k, n_same)
            body(Peer(lax.div(at, n_chip) * 2 + core, lax.rem(at, n_chip), at))
            return carry

        lax.fori_loop(1, n_same, step, 0)

    def on_core(k, body):
        pl.when(core == k)(body)

    def to_twin(src, dst, send, recv):
        on_core(0, lambda: remote(src, dst, send, recv, twin))

    def when_owner(body):
        on_core(1, body if n_own == n_same else lambda: pl.when(place < n_own)(body))

    def by_role(mine, theirs):
        if n_own == n_same:
            mine()
        else:
            pl.when(place < n_own)(mine)
            pl.when(place >= n_own)(theirs)

    def send_parts(src, came, both, dst, came_sem, send, recv):
        def body():
            landed(came, came_sem)
            both[...] = src[...] + came[...]

            def go(t):
                def copy():
                    remote(both.at[t.index], dst.at[place], send, recv, t)

                if n_own == n_same:
                    copy()
                else:
                    pl.when(t.index < n_own)(copy)

            same_core(go)

        on_core(1, body)

    def pass_on(layer):
        send_parts(
            rs.at[layer],
            ra.at[layer],
            rp.at[layer],
            rbuf.at[layer],
            ra_recv.at[layer],
            rs_send.at[layer],
            rs_recv.at[layer],
        )

    lane = lax.broadcasted_iota(jnp.int32, (1, 2 * ch), 1)

    def add_parts(layer):
        def body():
            landed(rbuf.at[layer, pl.ds(0, n_same - 1)], rs_recv.at[layer])
            rbuf[layer, place] = rp[layer, place]
            total = jnp.sum(rbuf[layer], axis=0)
            if layer in LINEAR:
                at = LINEAR.index(layer)
                landed(rxbuf.at[at, pl.ds(0, n_same - 1)], rx_recv.at[at])
                rxbuf[at, place] = rxp[at, place]
                extra = jnp.sum(rxbuf[at], axis=0)

                def mine(row, k):
                    first = 2 * (k * n_own + place)
                    even = jnp.sum(jnp.where(lane == first, row, 0.0), axis=1, keepdims=True)
                    odd = jnp.sum(jnp.where(lane == first + 1, row, 0.0), axis=1, keepdims=True)
                    return jnp.where(lane < ch, even, odd)

                sums = sigmas[layer]
                inv = pltpu.roll(sq[layer, 0:1, :], ch, axis=1)
                gain = par[11 + layer : 12 + layer, :]
                window = extra[9 * per : 9 * per + 9]
                parts = []
                for k in range(per):
                    c_dy = mine(sums / entries, k)
                    c_dx = mine(pltpu.roll(sums, ch, axis=1) / entries, k)
                    at = slice(9 * k, 9 * k + 9)
                    part = total[at] - c_dy * window - c_dx * extra[at]
                    parts.append(mine(gain * inv, k) * part)
                for k in range(per):
                    grads[layer, place, 9 * k : 9 * k + 9, :] = parts[k]
            else:
                grads[layer, place] = total
            out = grads.at[layer, place]
            same_core(lambda t: remote(out, out, ag_send.at[layer], ag_recv.at[layer], t))

        when_owner(body)

    def share(layer):
        def body():
            by_role(
                lambda: landed(grads.at[layer, pl.ds(0, n_own - 1)], ag_recv.at[layer]),
                lambda: landed(grads.at[layer], ag_recv.at[layer]),
            )
            whole = grads.at[layer]
            remote(whole, whole, sh_send.at[layer], sh_recv.at[layer], twin)

        on_core(1, body)

    for f in fetches[0:5]:
        f.wait()
    slot = lax.broadcasted_iota(jnp.int32, (maxp, pill), 0)
    per_sweep = []
    spots = []
    totals = [jnp.zeros((1, 1), F32)] * 9
    n_loc = jnp.zeros((1, 1), F32)
    for s in range(sweeps):
        valid = slot < counts[s : s + 1, :]
        mask = valid.astype(F32)
        cnt = counts[s : s + 1, :].astype(F32)
        sums = [jnp.sum(points[s, f] * mask, axis=0, keepdims=True) for f in range(4)]
        cents = [sums[f] / cnt for f in range(3)]
        cell = cells[s : s + 1, :]
        row = lax.shift_right_logical(cell, gw.bit_length() - 1)
        col = cell & (gw - 1)
        col_pos = col.astype(F32) * (2.0 / gw) - 1.0
        row_pos = row.astype(F32) * (2.0 / gh) - 1.0
        feats = sums + [sums[f] - cnt * cents[f] for f in range(3)]
        feats += [sums[0] - cnt * col_pos, sums[1] - cnt * row_pos]
        totals = [t + jnp.sum(f, axis=1, keepdims=True) for t, f in zip(totals, feats)]
        n_loc = n_loc + jnp.sum(cnt, axis=1, keepdims=True)
        per_sweep.append(cents + [col_pos, row_pos])
        spot = ((row & 1) * 2 + (col & 1)) * plane
        spot = spot + lax.shift_right_logical(row, 1) * w2 + lax.shift_right_logical(col, 1)
        spots.append(spot)
    for f in fetches[5:9]:
        f.wait()
    par[...] = jnp.zeros(par.shape, F32)
    par[0:9, 0:ch] = pw[...]
    par[9:10, 0:ch] = pfn_gain[...]
    par[10:11, 0:ch] = pfn_bias[...]
    par[11 : 11 + LAYERS, 0:ch] = bn_gain[...]
    par[11 + LAYERS : 11 + 2 * LAYERS, 0:ch] = bn_bias[...]
    par_cols = par[...].T
    pw_cols = par_cols[0:ch, 0:9]
    gain_c, bias_c = par_cols[0:ch, 9:10], par_cols[0:ch, 10:11]
    bn_cols = par_cols[0:ch, 11 : 11 + 2 * LAYERS]
    m_loc = jnp.zeros((ch, 1), F32)
    for f in range(9):
        m_loc = m_loc + pw_cols[:, f : f + 1] * totals[f]
    m_loc = m_loc / n_loc
    for s in range(sweeps):
        base = -m_loc
        for f in range(5):
            base = base - pw_cols[:, f + 4 : f + 5] * per_sweep[s][f]
        bm[s] = base

    def one_channel(c, carry):
        wx = pw_s[0, c] + pw_s[4, c] + pw_s[7, c]
        wy = pw_s[1, c] + pw_s[5, c] + pw_s[8, c]
        wz = pw_s[2, c] + pw_s[6, c]
        wr = pw_s[3, c]
        total = jnp.zeros((8, pill), F32)
        for s in range(sweeps):
            most = jnp.full((8, pill), LOWEST, F32)
            shift_by = bm[s, pl.ds(c, 1), :]
            have = counts[s : s + 1, :]
            for k in range(maxp // 8):
                part = pl.ds(8 * k, 8)
                ids = lax.broadcasted_iota(jnp.int32, (8, pill), 0) + 8 * k
                ok = ids < have
                h = points[s, 0, part, :] * wx + points[s, 1, part, :] * wy
                h = h + points[s, 2, part, :] * wz + points[s, 3, part, :] * wr + shift_by
                most = jnp.maximum(most, jnp.where(ok, h, LOWEST))
                h = jnp.where(ok, h, 0.0)
                total = total + h * h
            mx[s, c] = most
        folded = total[:, 0:128]
        for t in range(1, pill // 128):
            folded = folded + total[:, t * 128 : (t + 1) * 128]
        sq[c] = folded
        return carry

    lax.fori_loop(0, ch, one_channel, 0, unroll=4)
    both = jnp.concatenate([jnp.broadcast_to(m_loc, (ch, 128)), jnp.sum(sq[...], axis=1)], axis=0)
    turned = both.T
    row = jnp.where(lane < ch, turned[0:1, :], jnp.sum(turned, axis=0, keepdims=True))
    row = jnp.concatenate([row, jnp.broadcast_to(n_loc, (1, 2 * ch))], axis=1)

    pl.semaphore_wait(barrier, n - 1)
    send_row(st0, 0, row)

    col = lax.broadcasted_iota(jnp.int32, (1, w2), 1)
    tiles = pix // w2

    def tile(x, t):
        return x[:, t * w2 : (t + 1) * w2]

    def shift(x, d):
        if d == 0:
            return x
        ok = col >= -d if d < 0 else col < w2 - d
        return jnp.concatenate(
            [jnp.where(ok, pltpu.roll(tile(x, t), (-d) % w2, axis=1), 0.0) for t in range(tiles)],
            axis=1,
        )

    def down(x, d):
        parts = []
        for s in range(sweeps):
            for r in range(h2):
                inside = 0 <= r + d < h2
                t = s * h2 + r + d
                parts.append(tile(x, t) if inside else jnp.zeros((x.shape[0], w2), x.dtype))
        return jnp.concatenate(parts, axis=1)

    def stack_rows(at, per_tap):
        for a, (x, d) in enumerate(per_tap):
            for h in range(2):
                xs[at, h, a * ch : (a + 1) * ch, :] = down(x[h], d) if d else x[h]

    def stack_cols(ref, step, x, taps=3):
        for b in range(taps):
            for h, part in enumerate(split(shift(x, 1 - b))):
                ref[h * step + b * ch : h * step + (b + 1) * ch, :] = part

    def natural(layer):
        half = ch // 2
        for b in range(3):
            v = [w4[3 * a + b, :, layer, :] for a in range(3)]
            for k in range(2):
                v3 = [x[:, k * ch : (k + 1) * ch] for x in v]
                rows = pl.ds(b * ch + k, half, stride=2)
                wn[0, rows, :] = jnp.concatenate(v3[0:2], axis=1)
                wn[1, rows, :] = jnp.concatenate([v3[2], v3[2]], axis=1)
        return jnp.concatenate([wn[0], wn[1, :, 0:ch]], axis=1)

    def weights(layer):
        w = natural(layer)
        hi, lo = split(w)
        if layer == 0:
            for h, part in enumerate((hi, lo)):
                wfs[0, h * 2 * ch : (h * 2 + 1) * ch, :] = part[0:ch]
                wfs[0, (h * 2 + 1) * ch : (h * 2 + 2) * ch, :] = part[2 * ch : ch3]
                wfs[0, (4 + h) * ch : (5 + h) * ch, :] = part[ch : 2 * ch]
            first_backward_weights(w.T)
        else:
            wfs[layer, 0:ch3, :] = hi
            wfs[layer, ch3 : 2 * ch3, :] = lo
            hi, lo = split(w.T)
            wbs[layer - 1, 0:ch3, :] = hi
            wbs[layer - 1, ch3 : 2 * ch3, :] = lo

    def first_backward_weights(w):
        zero = jnp.zeros((ch, ch), F32)
        tap_of = {(0, 0): 1, (1, 0): 2, (1, 1): 0}
        for k in range(4):
            line = []
            for j in range(4):
                a, b = tap_of.get((k // 2, j // 2)), tap_of.get((k % 2, j % 2))
                none = a is None or b is None
                line.append(zero if none else w[a * ch : (a + 1) * ch, b * ch : (b + 1) * ch])
            hi, lo = split(jnp.concatenate(line, axis=1))
            wb0s[k * ch : (k + 1) * ch, :] = hi
            wb0s[(4 + k) * ch : (5 + k) * ch, :] = lo

    for s in range(sweeps):
        spot = jnp.broadcast_to(spots[s].astype(F32), (8, pill)).T[:, 0:1]
        for k in range(4):
            ids = lax.broadcasted_iota(jnp.int32, (pill, plane), 1) + k * plane
            hit = ids.astype(F32) == spot
            onehot[s, :, k * plane : (k + 1) * plane] = hit.astype(F32).astype(BF16)
    for s in range(sweeps):
        bm[s] = jnp.max(mx[s], axis=1)
    for f in fetches[9:11]:
        f.wait()
    weights(0)
    inside = lax.broadcasted_iota(jnp.int32, (16, pix), 0)
    cols = lax.broadcasted_iota(jnp.int32, (16, pix), 1) & (w2 - 1)
    ones = ((inside == 0) & (cols < w2 - 1)) | (inside == 1) | ((inside == 2) & (cols >= 1))
    hs[ch3 : ch3 + 16, :] = ones.astype(F32).astype(BF16)
    hs[2 * ch3 + 16 : 2 * ch3 + 32, :] = jnp.zeros((16, pix), BF16)

    def columns(row):
        turned = jnp.broadcast_to(row, (8, 2 * ch)).T
        return turned[0:ch, 0:1], turned[ch : 2 * ch, 0:1]

    got = wait_row(st0, 0)
    n_all = jnp.sum(got[:, :, 2 * ch :], axis=0)
    rows = got[:, :, 0 : 2 * ch]
    weighted = got[:, :, 2 * ch :]
    means = jnp.sum(rows * weighted, axis=0) / n_all
    dev = rows - means[None]
    spread = jnp.sum(dev * dev * weighted, axis=0)
    second = (jnp.sum(rows, axis=0) + pltpu.roll(spread, ch, axis=1)) / n_all
    mean_c, inv_c = columns(jnp.where(lane < ch, means, lax.rsqrt(second + EPS)))
    scale_c = gain_c * inv_c
    shift_c = scale_c * (m_loc - mean_c) + bias_c

    planes = [[], [], [], []]
    for s in range(sweeps):
        pillar = jnp.maximum(bm[s] * scale_c + shift_c, 0.0)
        hi, lo = split(pillar)
        placed = dot(jnp.concatenate([hi, lo], axis=0), onehot[s])
        for k in range(4):
            part = placed[:, k * plane : (k + 1) * plane]
            planes[k].append(part[0:ch] + part[ch : 2 * ch])
    planes = [split(jnp.concatenate(p, axis=1)) for p in planes]
    for k in range(2):
        stack_rows(k, [(planes[2 + k], -1), (planes[k], 0), (planes[2 + k], 0)])

    entries_loc = float(pix)
    entries = float(pix * n)

    def fold(x):
        out = x[:, 0:128]
        for t in range(1, pix // 128):
            out = out + x[:, t * 128 : (t + 1) * 128]
        return out

    def parts3(w, k, at):
        big = dot(w, xs[at, 0])
        return big[0:k] + big[k : 2 * k] + dot(w[0:k], xs[at, 1])

    def convolve(layer):
        if layer == 0:
            y = parts3(wfs[0, 0 : 4 * ch, :], 2 * ch, 1)
            return parts3(wfs[0, 4 * ch : 6 * ch, :], ch, 0) + y[ch : 2 * ch] + shift(y[0:ch], -1)
        y = parts3(wfs[layer], ch3, layer + 1)
        return y[ch : 2 * ch] + shift(y[0:ch], -1) + shift(y[2 * ch : ch3], 1)

    def correlate(both, k, at):
        big = dot(both, xs[at, 0], NT)
        return big[0:k] + big[k : 2 * k] + dot(both[0:k], xs[at, 1], NT)

    def pairs(store):
        half = ch // 2
        for b in range(3):
            for a in range(3):
                at = slice((a % 2) * ch, (a % 2 + 1) * ch)
                even = res[a // 2, pl.ds(b * ch, half, stride=2), :]
                odd = res[a // 2, pl.ds(b * ch + 1, half, stride=2), :]
                store(3 * a + b, jnp.concatenate([even[:, at], odd[:, at]], axis=1))

    def keep(at, x):
        res[0, at, :] = x[:, 0 : 2 * ch]
        res[1, at, 0:ch] = x[:, 2 * ch : ch3]

    def send_grad(ref, layer):
        if layer == 0:
            some = jnp.concatenate([ref[0 : 2 * ch, :], ref[ch3 : ch3 + 2 * ch, :]], axis=0)
            odd = correlate(some, 2 * ch, 1)
            some = jnp.concatenate([ref[ch : 2 * ch, :], ref[ch3 + ch : ch3 + 2 * ch, :]], axis=0)
            keep(slice(0, ch), odd[0:ch])
            keep(slice(ch, 2 * ch), correlate(some, ch, 0))
            keep(slice(2 * ch, ch3), odd[ch : 2 * ch])
        else:
            keep(slice(0, ch3), correlate(ref[...], ch3, layer + 1))

        def store(t, line):
            for k in range(per):
                rs[layer, :, 9 * k + t, :] = line[k * n_own : (k + 1) * n_own]

        pairs(store)
        to_twin(rs.at[layer], ra.at[layer], ra_send.at[layer], ra_recv.at[layer])

    def send_extra(layer):
        at = LINEAR.index(layer)
        k = ch3 + 16
        stack_cols(hs, k, xh[layer])
        if layer == 0:
            even, odd = correlate(hs[...], k, 0), correlate(hs[...], k, 1)
            keep(slice(0, ch), odd[0:ch])
            keep(slice(ch, 2 * ch), even[ch : 2 * ch])
            keep(slice(2 * ch, ch3), odd[ch : 2 * ch])
            window = [odd[ch3 : ch3 + 1], even[ch3 + 1 : ch3 + 2], odd[ch3 + 1 : ch3 + 2]]
        else:
            both = correlate(hs[...], k, layer + 1)
            keep(slice(0, ch3), both[0:ch3])
            window = [both[ch3 + b : ch3 + b + 1] for b in range(3)]

        def store(t, line):
            for k in range(per):
                rx[at, :, 9 * k + t, :] = line[k * n_own : (k + 1) * n_own]

        pairs(store)
        for b in range(3):
            for a in range(3):
                one = window[b][:, a * ch : (a + 1) * ch]
                line = jnp.concatenate([one, one], axis=1)
                rx[at, :, 9 * per + 3 * a + b, :] = jnp.broadcast_to(line, (n_own, 2 * ch))
        to_twin(rx.at[at], rxa.at[at], rxa_send.at[at], rxa_recv.at[at])

    def pass_extra(layer):
        at = LINEAR.index(layer)
        send_parts(
            rx.at[at],
            rxa.at[at],
            rxp.at[at],
            rxbuf.at[at],
            rxa_recv.at[at],
            rx_send.at[at],
            rx_recv.at[at],
        )

    def finish(layer):
        scale, off, inv, by = affine[layer]
        d = xh[layer]
        y = scale * d + off
        xh[layer] = inv * (d - by)
        sig = jax.nn.sigmoid(y)
        yy[layer] = sig * (1.0 + y * (1.0 - sig))

    affine = []
    sigmas = {}
    act = None
    for layer in range(LAYERS):
        z = convolve(layer)
        sums = fold(z)
        m_loc = jnp.sum(sums, axis=1, keepdims=True) / entries_loc
        d = z - m_loc
        turned = jnp.concatenate([sums, fold(d * d)], axis=0).T
        row = jnp.sum(turned, axis=0, keepdims=True)
        row = jnp.where(lane < ch, row / entries_loc, row)
        send_row(st, layer + 1, row)
        xh[layer] = d
        if layer - 2 in LINEAR:
            pass_extra(layer - 2)
        if layer + 1 < LAYERS:
            weights(layer + 1)
        else:
            for s in range(sweeps):
                for r in range(h2):
                    at = s * plane + r * w2
                    cot_s[:, at : at + w2] = cot[s, :, r, :]
        if layer > 0:
            finish(layer - 1)
            if layer - 1 in LINEAR:
                send_extra(layer - 1)
        rows = wait_row(st, layer + 1)
        total = jnp.sum(rows, axis=0)
        means = total / float(n)
        dev = rows - means[None]
        spread = jnp.sum(dev * dev, axis=0) * entries_loc
        second = (total + pltpu.roll(spread, ch, axis=1)) / entries
        row = jnp.where(lane < ch, means, lax.rsqrt(second + EPS))
        mean_c, inv_c = columns(row)
        sq[layer, :, :] = jnp.broadcast_to(row, (8, 2 * ch))
        by = mean_c - m_loc
        scale = bn_cols[:, layer : layer + 1] * inv_c
        off = bn_cols[:, LAYERS + layer : LAYERS + layer + 1] - scale * by
        affine.append((scale, off, inv_c, by))
        y = scale * xh[layer] + off
        act = y * jax.nn.sigmoid(y)
        if layer + 1 < LAYERS:
            hi_lo = split(act)
            stack_rows(layer + 2, [(hi_lo, -1), (hi_lo, 0), (hi_lo, 1)])
        else:
            finish(layer)

    def backward(layer):
        w = wbs[layer - 1]
        big = dot(w, gs[0:ch3, :])
        v = big[0:ch3] + big[ch3 : 2 * ch3] + dot(w[0:ch3], gs[ch3 : 2 * ch3, :])
        return v[ch : 2 * ch] + down(v[0:ch], 1) + down(v[2 * ch : ch3], -1)

    u = cot_s[...]
    for layer in range(LAYERS - 1, -1, -1):
        gy = u * yy[layer]
        turned = jnp.concatenate([fold(gy), fold(gy * xh[layer])], axis=0).T
        rnd = 2 * LAYERS - layer
        send_row(st, rnd, jnp.sum(turned, axis=0, keepdims=True))
        if layer == LAYERS - 1:
            for s in range(sweeps):
                for r in range(h2):
                    at = s * plane + r * w2
                    feat[s, :, r, :] = act[:, at : at + w2]
        if layer in LINEAR:
            stack_cols(hs, ch3, gy, 2 if layer == 0 else 3)
            send_grad(hs.at[0 : 2 * ch3, :], layer)
        if layer + 1 < LAYERS and layer + 1 not in LINEAR:
            send_grad(gs, layer + 1)
        if layer in LINEAR:
            pass_on(layer)
        if layer == 0:
            share(LAYERS - 1)
        for done in range(LAYERS - 1, layer, -1):
            if done == layer + (1 if done in LINEAR else 2):
                add_parts(done)
        if layer + 1 < LAYERS and layer + 1 not in LINEAR:
            pass_on(layer + 1)
        row = jnp.sum(wait_row(st, rnd), axis=0)
        sigmas[layer] = row
        norms[0, layer : layer + 1, :] = row[:, ch : 2 * ch]
        norms[1, layer : layer + 1, :] = row[:, 0:ch]
        dy_c, dyx_c = columns(row / entries)
        gz = affine[layer][0] * (gy - dy_c - xh[layer] * dyx_c)
        if layer > 0:
            stack_cols(gs, ch3, gz)
            u = backward(layer)
    for dr in range(2):
        for dc in range(2):
            hi, lo = split(shift(down(gz, dr), dc))
            at = pl.ds((2 * dr + dc) * ch, ch)
            g4[0, at, :] = hi
            g4[1, at, :] = lo
    big = dot(wb0s[...], g4[0])
    u0 = big[0 : 4 * ch] + big[4 * ch :] + dot(wb0s[0 : 4 * ch, :], g4[1])
    for s in range(sweeps):
        total = None
        for k in range(4):
            hi, lo = split(u0[k * ch : (k + 1) * ch, s * plane : (s + 1) * plane])
            both = jnp.concatenate([hi, lo], axis=0)
            part = dot(both, onehot[s, :, k * plane : (k + 1) * plane], NT)
            total = part if total is None else total + part
        pgrad[s] = total[0:ch] + total[ch : 2 * ch]
    add_parts(0)

    def arrived(layer):
        on_core(0, lambda: landed(grads.at[layer], sh_recv.at[layer]))

    def unpack(layer):
        arrived(layer)
        for t in range(9):
            for k in range(per):
                part = grads[layer, :, 9 * k + t, :]
                out_g[t, k * n_own : (k + 1) * n_own, layer, :] = part

    def sent(ref, sem):
        by_role(lambda: landed(ref.at[pl.ds(0, n_own - 1)], sem), lambda: landed(ref, sem))

    def drain(layer):
        on_core(0, lambda: landed(ra.at[layer], ra_send.at[layer]))
        on_core(1, lambda: sent(rp.at[layer], rs_send.at[layer]))
        when_owner(lambda: landed(rbuf.at[layer, pl.ds(0, n_same - 1)], ag_send.at[layer]))

    for layer in range(LAYERS - 2, 0, -1):
        share(layer)
    for rnd in range(2 * LAYERS + 1):
        landed((st0.at[0] if rnd == 0 else st.at[rnd]).at[pl.ds(0, n - 1)], st_send.at[rnd])
    for at in range(len(LINEAR)):
        on_core(0, lambda: landed(rxa.at[at], rxa_send.at[at]))
        on_core(1, lambda: sent(rxp.at[at], rx_send.at[at]))
    for layer in range(LAYERS - 1, 0, -1):
        unpack(layer)
        drain(layer)
    share(0)
    drain(0)
    unpack(0)

    def shared():
        for layer in range(LAYERS):
            landed(grads.at[layer], sh_send.at[layer])

    on_core(1, shared)


def write_out(a, b, c, d, a_h, b_h, c_h, d_h, sem):
    pairs = [(b, b_h), (a, a_h), (d, d_h), (c, c_h)]
    copies = [pltpu.make_async_copy(x, y, sem.at[i]) for i, (x, y) in enumerate(pairs)]
    for x in copies:
        x.start()
    for x in copies:
        x.wait()


def per_device(
    n_rack,
    n_chip,
    points,
    counts,
    cells,
    pfn_weight,
    pfn_gain,
    pfn_bias,
    conv_weight,
    bn_gain,
    bn_bias,
    cotangent,
):
    sweeps, _, maxp, pill = points.shape
    ch = pfn_weight.shape[1]
    h2, w2 = cotangent.shape[2:]
    gh, gw = 2 * h2, 2 * w2
    n = n_rack * n_chip
    owners = ch // 2
    n_own = min(n // 2, owners)
    per = owners // n_own
    assert owners % n_own == 0 and n_rack % 2 == 0 and w2 == 128 and 2 * ch == 128
    pix = sweeps * h2 * w2
    ch3 = 3 * ch
    dims = (n_rack, n_chip, sweeps, maxp, gh, gw, pill, ch, owners)
    hbm = pl.BlockSpec(memory_space=pl.ANY)
    vmem = pl.BlockSpec(memory_space=pltpu.VMEM)
    extra = len(LINEAR)
    w4 = conv_weight.reshape(LAYERS, 9, owners, 2 * ch).transpose(1, 2, 0, 3)
    dma = pltpu.SemaphoreType.DMA
    outs = pl.pallas_call(
        functools.partial(kernel, dims),
        out_shape=(
            pltpu.VMEM((sweeps, ch, h2, w2), F32),
            pltpu.VMEM((9, owners, LAYERS, 2 * ch), F32),
            pltpu.VMEM((2, LAYERS, ch), F32),
            pltpu.VMEM((sweeps, ch, pill), F32),
        ),
        in_specs=[hbm] * 10,
        out_specs=(vmem,) * 4,
        scratch_shapes=[
            pltpu.VMEM((sweeps, 4, maxp, pill), F32),
            pltpu.VMEM((sweeps, pill), jnp.int32),
            pltpu.VMEM((sweeps, pill), jnp.int32),
            pltpu.VMEM((9, ch), F32),
            pltpu.SMEM((9, ch), F32),
            pltpu.VMEM((1, ch), F32),
            pltpu.VMEM((1, ch), F32),
            pltpu.VMEM((9, owners, LAYERS, 2 * ch), F32),
            pltpu.VMEM((LAYERS, ch), F32),
            pltpu.VMEM((LAYERS, ch), F32),
            pltpu.VMEM((sweeps, ch, h2, w2), F32),
            pltpu.VMEM((LAYERS + 1, 2, ch3, pix), BF16),
            pltpu.VMEM((2 * ch3, pix), BF16),
            pltpu.VMEM((2 * ch3 + 32, pix), BF16),
            pltpu.VMEM((2, ch3, 2 * ch), F32),
            pltpu.VMEM((2, ch3, 2 * ch), F32),
            pltpu.VMEM((LAYERS, 2 * ch3, ch3), BF16),
            pltpu.VMEM((LAYERS - 1, 2 * ch3, ch3), BF16),
            pltpu.VMEM((8 * ch, 4 * ch), BF16),
            pltpu.VMEM((2, 4 * ch, pix), BF16),
            pltpu.VMEM((sweeps, pill, gh * gw), BF16),
            pltpu.VMEM((32, 128), F32),
            pltpu.VMEM((ch, pix), F32),
            pltpu.VMEM((LAYERS, n_own, 9 * per, 2 * ch), F32),
            pltpu.VMEM((sweeps, ch, pill), F32),
            pltpu.VMEM((sweeps, ch, 8, pill), F32),
            pltpu.VMEM((ch, 8, 128), F32),
            pltpu.VMEM((LAYERS, ch, pix), F32),
            pltpu.VMEM((LAYERS, ch, pix), F32),
            pltpu.VMEM((1, n, 1, 4 * ch), F32),
            pltpu.VMEM((2 * LAYERS + 1, n, 1, 2 * ch), F32),
            pltpu.VMEM((LAYERS, n_own, 9 * per, 2 * ch), F32),
            pltpu.VMEM((LAYERS, n_own, 9 * per, 2 * ch), F32),
            pltpu.VMEM((LAYERS, n_own, 9 * per, 2 * ch), F32),
            pltpu.VMEM((LAYERS, n // 2, 9 * per, 2 * ch), F32),
            pltpu.VMEM((extra, n_own, 9 * per + 9, 2 * ch), F32),
            pltpu.VMEM((extra, n_own, 9 * per + 9, 2 * ch), F32),
            pltpu.VMEM((extra, n_own, 9 * per + 9, 2 * ch), F32),
            pltpu.VMEM((extra, n // 2, 9 * per + 9, 2 * ch), F32),
            dma((11,)),
            dma((2 * LAYERS + 1,)),
            dma((2 * LAYERS + 1,)),
            dma((LAYERS,)),
            dma((LAYERS,)),
            dma((LAYERS,)),
            dma((LAYERS,)),
            dma((extra,)),
            dma((extra,)),
            dma((extra,)),
            dma((extra,)),
            dma((LAYERS,)),
            dma((LAYERS,)),
            dma((LAYERS,)),
            dma((LAYERS,)),
        ],
        compiler_params=pltpu.CompilerParams(
            collective_id=0, has_side_effects=True, vmem_limit_bytes=56 * 1024 * 1024
        ),
    )(
        points,
        counts,
        cells,
        pfn_weight,
        pfn_gain.reshape(1, ch),
        pfn_bias.reshape(1, ch),
        w4,
        bn_gain,
        bn_bias,
        cotangent,
    )
    feat, out_g, norms, pgrad = pl.pallas_call(
        write_out,
        out_shape=tuple(jax.ShapeDtypeStruct(x.shape, x.dtype) for x in outs),
        in_specs=[vmem] * 4,
        out_specs=(hbm,) * 4,
        scratch_shapes=[dma((4,))],
    )(*[pltpu.with_memory_space_constraint(x, pltpu.VMEM) for x in outs])
    grads = out_g.transpose(2, 0, 1, 3).reshape(LAYERS, 9, ch * ch)
    return (feat, grads, norms, pgrad)


def solution(mesh):
    both = ("rack", "chip")
    return jax.shard_map(
        functools.partial(per_device, mesh.shape["rack"], mesh.shape["chip"]),
        mesh=mesh,
        in_specs=(
            P(both, None, None, None),
            P(both, None),
            P(both, None),
            P(),
            P(),
            P(),
            P(),
            P(),
            P(),
            P(both, None, None, None),
        ),
        out_specs=(
            P(both, None, None, None),
            P(),
            P(),
            P(both, None, None),
        ),
        check_vma=False,
    )
```

```python
import functools

import jax
import jax.numpy as jnp
from jax import lax
from jax.experimental import pallas as pl
from jax.experimental.pallas import tpu as pltpu
from jax.sharding import PartitionSpec as P

LAYERS = 4
LINEAR = (0, 1)
EPS = 1e-05
F32 = jnp.float32
BF16 = jnp.bfloat16
NN = (((1,), (0,)), ((), ()))
NT = (((1,), (1,)), ((), ()))
LOWEST = -3e38


class Peer:
    def __init__(self, rack, chip, index):
        self.rack, self.chip, self.index = rack, chip, index


def dot(a, b, dims=NN):
    return lax.dot_general(a, b, dims, preferred_element_type=F32)


def split(x):
    hi = x.astype(BF16)
    lo = (x - hi.astype(F32)).astype(BF16)
    return hi, lo


def kernel(
    dims,
    points_h,
    counts_h,
    cells_h,
    pw_h,
    pfn_gain_h,
    pfn_bias_h,
    w4_h,
    bn_gain_h,
    bn_bias_h,
    cot_h,
    feat,
    out_g,
    norms,
    pgrad,
    points,
    counts,
    cells,
    pw,
    pw_s,
    pfn_gain,
    pfn_bias,
    w4,
    bn_gain,
    bn_bias,
    cot,
    xs,
    gs,
    hs,
    res,
    wn,
    wfs,
    wbs,
    wb0s,
    g4,
    onehot,
    par,
    cot_s,
    grads,
    bm,
    mx,
    sq,
    xh,
    yy,
    st0,
    st,
    rs,
    ra,
    rp,
    rbuf,
    rx,
    rxa,
    rxp,
    rxbuf,
    in_sem,
    st_send,
    st_recv,
    ra_send,
    ra_recv,
    rs_send,
    rs_recv,
    rxa_send,
    rxa_recv,
    rx_send,
    rx_recv,
    ag_send,
    ag_recv,
    sh_send,
    sh_recv,
):
    n_rack, n_chip, sweeps, maxp, gh, gw, pill, ch, owners = dims
    n = n_rack * n_chip
    h2, w2 = gh // 2, gw // 2
    plane = h2 * w2
    pix = sweeps * plane
    ch3 = 3 * ch
    my_rack, my_chip = lax.axis_index("rack"), lax.axis_index("chip")
    me = my_rack * n_chip + my_chip
    n_same = n // 2
    n_own = min(n_same, owners)
    per = owners // n_own
    core, my_x = lax.rem(my_rack, 2), lax.div(my_rack, 2)
    place = my_x * n_chip + my_chip
    twin = Peer(my_rack + 1 - 2 * core, my_chip, 0)

    fetches = [
        (points_h, points),
        (counts_h, counts),
        (cells_h, cells),
        (pw_h, pw),
        (pw_h, pw_s),
        (pfn_gain_h, pfn_gain),
        (pfn_bias_h, pfn_bias),
        (bn_gain_h, bn_gain),
        (bn_bias_h, bn_bias),
        (w4_h, w4),
        (cot_h, cot),
    ]
    fetches = [pltpu.make_async_copy(a, b, in_sem.at[i]) for i, (a, b) in enumerate(fetches)]

    def device(t):
        if isinstance(t, Peer):
            return {"rack": t.rack, "chip": t.chip}
        return {"rack": lax.div(t, n_chip), "chip": lax.rem(t, n_chip)}

    def flipped(x, size):
        out = []
        for m in range(size):
            y = x
            for bit in (1, 2, 4, 8, 16):
                if m & bit:
                    y = y + bit * (1 - 2 * lax.rem(lax.div(x, bit), 2))
            out.append(y)
        return out

    def is_power(k):
        return k & (k - 1) == 0

    few = n <= 32 and is_power(n_rack) and is_power(n_chip)
    if few:
        racks, chips = flipped(my_rack, n_rack), flipped(my_chip, n_chip)

    def far(k):
        r, c = divmod(k, n_chip)
        return -(c // 2 + c % 2 + r // 2 + 0.3 * (r % 2))

    def peers(body):
        if few:
            for k in sorted(range(1, n), key=far):
                r, c = divmod(k, n_chip)
                body(Peer(racks[r], chips[c], racks[r] * n_chip + chips[c]))
            return

        def step(k, carry):
            body(lax.rem(me + k, n))
            return carry

        lax.fori_loop(1, n, step, 0)

    for f in fetches:
        f.start()
    barrier = pltpu.get_barrier_semaphore()
    peers(
        lambda t: pl.semaphore_signal(
            barrier, inc=1, device_id=device(t), device_id_type=pl.DeviceIdType.MESH
        )
    )

    def remote(src, dst, send, recv, t):
        pltpu.make_async_remote_copy(
            src_ref=src,
            dst_ref=dst,
            send_sem=send,
            recv_sem=recv,
            device_id=device(t),
            device_id_type=pl.DeviceIdType.MESH,
        ).start()

    def landed(ref, sem):
        pltpu.make_async_copy(ref, ref, sem).wait()

    def send_row(buf, rnd, row):
        buf[rnd, me] = row
        mine = buf.at[rnd, me]
        peers(lambda t: remote(mine, mine, st_send.at[rnd], st_recv.at[rnd], t))

    def wait_row(buf, rnd):
        landed(buf.at[rnd, pl.ds(0, n - 1)], st_recv.at[rnd])
        return buf[rnd]

    def same_core(body):
        if few:
            for k in sorted(range(n), key=far):
                r, c = divmod(k, n_chip)
                if k > 0 and r % 2 == 0:
                    x = lax.div(racks[r], 2)
                    body(Peer(racks[r], chips[c], x * n_chip + chips[c]))
            return

        def step(k, carry):
            at = lax.rem(place + k, n_same)
            body(Peer(lax.div(at, n_chip) * 2 + core, lax.rem(at, n_chip), at))
            return carry

        lax.fori_loop(1, n_same, step, 0)

    def on_core(k, body):
        pl.when(core == k)(body)

    def to_twin(src, dst, send, recv):
        on_core(0, lambda: remote(src, dst, send, recv, twin))

    def when_owner(body):
        on_core(1, body if n_own == n_same else lambda: pl.when(place < n_own)(body))

    def by_role(mine, theirs):
        if n_own == n_same:
            mine()
        else:
            pl.when(place < n_own)(mine)
            pl.when(place >= n_own)(theirs)

    def send_parts(src, came, both, dst, came_sem, send, recv):
        def body():
            landed(came, came_sem)
            both[...] = src[...] + came[...]

            def go(t):
                def copy():
                    remote(both.at[t.index], dst.at[place], send, recv, t)

                if n_own == n_same:
                    copy()
                else:
                    pl.when(t.index < n_own)(copy)

            same_core(go)

        on_core(1, body)

    def pass_on(layer):
        send_parts(
            rs.at[layer],
            ra.at[layer],
            rp.at[layer],
            rbuf.at[layer],
            ra_recv.at[layer],
            rs_send.at[layer],
            rs_recv.at[layer],
        )

    lane = lax.broadcasted_iota(jnp.int32, (1, 2 * ch), 1)

    def add_parts(layer):
        def body():
            landed(rbuf.at[layer, pl.ds(0, n_same - 1)], rs_recv.at[layer])
            rbuf[layer, place] = rp[layer, place]
            total = jnp.sum(rbuf[layer], axis=0)
            if layer in LINEAR:
                at = LINEAR.index(layer)
                landed(rxbuf.at[at, pl.ds(0, n_same - 1)], rx_recv.at[at])
                rxbuf[at, place] = rxp[at, place]
                extra = jnp.sum(rxbuf[at], axis=0)

                def mine(row, k):
                    first = 2 * (k * n_own + place)
                    even = jnp.sum(jnp.where(lane == first, row, 0.0), axis=1, keepdims=True)
                    odd = jnp.sum(jnp.where(lane == first + 1, row, 0.0), axis=1, keepdims=True)
                    return jnp.where(lane < ch, even, odd)

                sums = sigmas[layer]
                inv = pltpu.roll(sq[layer, 0:1, :], ch, axis=1)
                gain = par[11 + layer : 12 + layer, :]
                window = extra[9 * per : 9 * per + 9]
                parts = []
                for k in range(per):
                    c_dy = mine(sums / entries, k)
                    c_dx = mine(pltpu.roll(sums, ch, axis=1) / entries, k)
                    at = slice(9 * k, 9 * k + 9)
                    part = total[at] - c_dy * window - c_dx * extra[at]
                    parts.append(mine(gain * inv, k) * part)
                for k in range(per):
                    grads[layer, place, 9 * k : 9 * k + 9, :] = parts[k]
            else:
                grads[layer, place] = total
            out = grads.at[layer, place]
            same_core(lambda t: remote(out, out, ag_send.at[layer], ag_recv.at[layer], t))

        when_owner(body)

    def share(layer):
        def body():
            by_role(
                lambda: landed(grads.at[layer, pl.ds(0, n_own - 1)], ag_recv.at[layer]),
                lambda: landed(grads.at[layer], ag_recv.at[layer]),
            )
            whole = grads.at[layer]
            remote(whole, whole, sh_send.at[layer], sh_recv.at[layer], twin)

        on_core(1, body)

    for f in fetches[0:5]:
        f.wait()
    slot = lax.broadcasted_iota(jnp.int32, (maxp, pill), 0)
    per_sweep = []
    spots = []
    totals = [jnp.zeros((1, 1), F32)] * 9
    n_loc = jnp.zeros((1, 1), F32)
    for s in range(sweeps):
        valid = slot < counts[s : s + 1, :]
        mask = valid.astype(F32)
        cnt = counts[s : s + 1, :].astype(F32)
        sums = [jnp.sum(points[s, f] * mask, axis=0, keepdims=True) for f in range(4)]
        cents = [sums[f] / cnt for f in range(3)]
        cell = cells[s : s + 1, :]
        row = lax.shift_right_logical(cell, gw.bit_length() - 1)
        col = cell & (gw - 1)
        col_pos = col.astype(F32) * (2.0 / gw) - 1.0
        row_pos = row.astype(F32) * (2.0 / gh) - 1.0
        feats = sums + [sums[f] - cnt * cents[f] for f in range(3)]
        feats += [sums[0] - cnt * col_pos, sums[1] - cnt * row_pos]
        totals = [t + jnp.sum(f, axis=1, keepdims=True) for t, f in zip(totals, feats)]
        n_loc = n_loc + jnp.sum(cnt, axis=1, keepdims=True)
        per_sweep.append(cents + [col_pos, row_pos])
        spot = ((row & 1) * 2 + (col & 1)) * plane
        spot = spot + lax.shift_right_logical(row, 1) * w2 + lax.shift_right_logical(col, 1)
        spots.append(spot)
    for f in fetches[5:9]:
        f.wait()
    par[...] = jnp.zeros(par.shape, F32)
    par[0:9, 0:ch] = pw[...]
    par[9:10, 0:ch] = pfn_gain[...]
    par[10:11, 0:ch] = pfn_bias[...]
    par[11 : 11 + LAYERS, 0:ch] = bn_gain[...]
    par[11 + LAYERS : 11 + 2 * LAYERS, 0:ch] = bn_bias[...]
    par_cols = par[...].T
    pw_cols = par_cols[0:ch, 0:9]
    gain_c, bias_c = par_cols[0:ch, 9:10], par_cols[0:ch, 10:11]
    bn_cols = par_cols[0:ch, 11 : 11 + 2 * LAYERS]
    m_loc = jnp.zeros((ch, 1), F32)
    for f in range(9):
        m_loc = m_loc + pw_cols[:, f : f + 1] * totals[f]
    m_loc = m_loc / n_loc
    for s in range(sweeps):
        base = -m_loc
        for f in range(5):
            base = base - pw_cols[:, f + 4 : f + 5] * per_sweep[s][f]
        bm[s] = base

    def one_channel(c, carry):
        wx = pw_s[0, c] + pw_s[4, c] + pw_s[7, c]
        wy = pw_s[1, c] + pw_s[5, c] + pw_s[8, c]
        wz = pw_s[2, c] + pw_s[6, c]
        wr = pw_s[3, c]
        total = jnp.zeros((8, pill), F32)
        for s in range(sweeps):
            most = jnp.full((8, pill), LOWEST, F32)
            shift_by = bm[s, pl.ds(c, 1), :]
            have = counts[s : s + 1, :]
            for k in range(maxp // 8):
                part = pl.ds(8 * k, 8)
                ids = lax.broadcasted_iota(jnp.int32, (8, pill), 0) + 8 * k
                ok = ids < have
                h = points[s, 0, part, :] * wx + points[s, 1, part, :] * wy
                h = h + points[s, 2, part, :] * wz + points[s, 3, part, :] * wr + shift_by
                most = jnp.maximum(most, jnp.where(ok, h, LOWEST))
                h = jnp.where(ok, h, 0.0)
                total = total + h * h
            mx[s, c] = most
        folded = total[:, 0:128]
        for t in range(1, pill // 128):
            folded = folded + total[:, t * 128 : (t + 1) * 128]
        sq[c] = folded
        return carry

    lax.fori_loop(0, ch, one_channel, 0, unroll=8)
    both = jnp.concatenate([jnp.broadcast_to(m_loc, (ch, 128)), jnp.sum(sq[...], axis=1)], axis=0)
    turned = both.T
    row = jnp.where(lane < ch, turned[0:1, :], jnp.sum(turned, axis=0, keepdims=True))
    row = jnp.concatenate([row, jnp.broadcast_to(n_loc, (1, 2 * ch))], axis=1)

    pl.semaphore_wait(barrier, n - 1)
    send_row(st0, 0, row)

    col = lax.broadcasted_iota(jnp.int32, (1, w2), 1)
    tiles = pix // w2

    def tile(x, t):
        return x[:, t * w2 : (t + 1) * w2]

    def shift(x, d):
        if d == 0:
            return x
        ok = col >= -d if d < 0 else col < w2 - d
        return jnp.concatenate(
            [jnp.where(ok, pltpu.roll(tile(x, t), (-d) % w2, axis=1), 0.0) for t in range(tiles)],
            axis=1,
        )

    def down(x, d):
        parts = []
        for s in range(sweeps):
            for r in range(h2):
                inside = 0 <= r + d < h2
                t = s * h2 + r + d
                parts.append(tile(x, t) if inside else jnp.zeros((x.shape[0], w2), x.dtype))
        return jnp.concatenate(parts, axis=1)

    def stack_rows(at, per_tap):
        for a, (x, d) in enumerate(per_tap):
            for h in range(2):
                xs[at, h, a * ch : (a + 1) * ch, :] = down(x[h], d) if d else x[h]

    def stack_cols(ref, step, x, taps=3):
        for b in range(taps):
            for h, part in enumerate(split(shift(x, 1 - b))):
                ref[h * step + b * ch : h * step + (b + 1) * ch, :] = part

    def natural(layer):
        half = ch // 2
        for b in range(3):
            v = [w4[3 * a + b, :, layer, :] for a in range(3)]
            for k in range(2):
                v3 = [x[:, k * ch : (k + 1) * ch] for x in v]
                rows = pl.ds(b * ch + k, half, stride=2)
                wn[0, rows, :] = jnp.concatenate(v3[0:2], axis=1)
                wn[1, rows, :] = jnp.concatenate([v3[2], v3[2]], axis=1)
        return jnp.concatenate([wn[0], wn[1, :, 0:ch]], axis=1)

    def weights(layer):
        w = natural(layer)
        hi, lo = split(w)
        if layer == 0:
            for h, part in enumerate((hi, lo)):
                wfs[0, h * 2 * ch : (h * 2 + 1) * ch, :] = part[0:ch]
                wfs[0, (h * 2 + 1) * ch : (h * 2 + 2) * ch, :] = part[2 * ch : ch3]
                wfs[0, (4 + h) * ch : (5 + h) * ch, :] = part[ch : 2 * ch]
            first_backward_weights(w.T)
        else:
            wfs[layer, 0:ch3, :] = hi
            wfs[layer, ch3 : 2 * ch3, :] = lo
            hi, lo = split(w.T)
            wbs[layer - 1, 0:ch3, :] = hi
            wbs[layer - 1, ch3 : 2 * ch3, :] = lo

    def first_backward_weights(w):
        zero = jnp.zeros((ch, ch), F32)
        tap_of = {(0, 0): 1, (1, 0): 2, (1, 1): 0}
        for k in range(4):
            line = []
            for j in range(4):
                a, b = tap_of.get((k // 2, j // 2)), tap_of.get((k % 2, j % 2))
                none = a is None or b is None
                line.append(zero if none else w[a * ch : (a + 1) * ch, b * ch : (b + 1) * ch])
            hi, lo = split(jnp.concatenate(line, axis=1))
            wb0s[k * ch : (k + 1) * ch, :] = hi
            wb0s[(4 + k) * ch : (5 + k) * ch, :] = lo

    for s in range(sweeps):
        spot = jnp.broadcast_to(spots[s].astype(F32), (8, pill)).T[:, 0:1]
        for k in range(4):
            ids = lax.broadcasted_iota(jnp.int32, (pill, plane), 1) + k * plane
            hit = ids.astype(F32) == spot
            onehot[s, :, k * plane : (k + 1) * plane] = hit.astype(F32).astype(BF16)
    for s in range(sweeps):
        bm[s] = jnp.max(mx[s], axis=1)
    for f in fetches[9:11]:
        f.wait()
    weights(0)
    inside = lax.broadcasted_iota(jnp.int32, (16, pix), 0)
    cols = lax.broadcasted_iota(jnp.int32, (16, pix), 1) & (w2 - 1)
    ones = ((inside == 0) & (cols < w2 - 1)) | (inside == 1) | ((inside == 2) & (cols >= 1))
    hs[ch3 : ch3 + 16, :] = ones.astype(F32).astype(BF16)
    hs[2 * ch3 + 16 : 2 * ch3 + 32, :] = jnp.zeros((16, pix), BF16)

    def columns(row):
        turned = jnp.broadcast_to(row, (8, 2 * ch)).T
        return turned[0:ch, 0:1], turned[ch : 2 * ch, 0:1]

    got = wait_row(st0, 0)
    n_all = jnp.sum(got[:, :, 2 * ch :], axis=0)
    rows = got[:, :, 0 : 2 * ch]
    weighted = got[:, :, 2 * ch :]
    means = jnp.sum(rows * weighted, axis=0) / n_all
    dev = rows - means[None]
    spread = jnp.sum(dev * dev * weighted, axis=0)
    second = (jnp.sum(rows, axis=0) + pltpu.roll(spread, ch, axis=1)) / n_all
    mean_c, inv_c = columns(jnp.where(lane < ch, means, lax.rsqrt(second + EPS)))
    scale_c = gain_c * inv_c
    shift_c = scale_c * (m_loc - mean_c) + bias_c

    planes = [[], [], [], []]
    for s in range(sweeps):
        pillar = jnp.maximum(bm[s] * scale_c + shift_c, 0.0)
        hi, lo = split(pillar)
        placed = dot(jnp.concatenate([hi, lo], axis=0), onehot[s])
        for k in range(4):
            part = placed[:, k * plane : (k + 1) * plane]
            planes[k].append(part[0:ch] + part[ch : 2 * ch])
    planes = [split(jnp.concatenate(p, axis=1)) for p in planes]
    for k in range(2):
        stack_rows(k, [(planes[2 + k], -1), (planes[k], 0), (planes[2 + k], 0)])

    entries_loc = float(pix)
    entries = float(pix * n)

    def fold(x):
        out = x[:, 0:128]
        for t in range(1, pix // 128):
            out = out + x[:, t * 128 : (t + 1) * 128]
        return out

    def parts3(w, k, at):
        big = dot(w, xs[at, 0])
        return big[0:k] + big[k : 2 * k] + dot(w[0:k], xs[at, 1])

    def convolve(layer):
        if layer == 0:
            y = parts3(wfs[0, 0 : 4 * ch, :], 2 * ch, 1)
            return parts3(wfs[0, 4 * ch : 6 * ch, :], ch, 0) + y[ch : 2 * ch] + shift(y[0:ch], -1)
        y = parts3(wfs[layer], ch3, layer + 1)
        return y[ch : 2 * ch] + shift(y[0:ch], -1) + shift(y[2 * ch : ch3], 1)

    def correlate(both, k, at):
        big = dot(both, xs[at, 0], NT)
        return big[0:k] + big[k : 2 * k] + dot(both[0:k], xs[at, 1], NT)

    def pairs(store):
        half = ch // 2
        for b in range(3):
            for a in range(3):
                at = slice((a % 2) * ch, (a % 2 + 1) * ch)
                even = res[a // 2, pl.ds(b * ch, half, stride=2), :]
                odd = res[a // 2, pl.ds(b * ch + 1, half, stride=2), :]
                store(3 * a + b, jnp.concatenate([even[:, at], odd[:, at]], axis=1))

    def keep(at, x):
        res[0, at, :] = x[:, 0 : 2 * ch]
        res[1, at, 0:ch] = x[:, 2 * ch : ch3]

    def send_grad(ref, layer):
        if layer == 0:
            some = jnp.concatenate([ref[0 : 2 * ch, :], ref[ch3 : ch3 + 2 * ch, :]], axis=0)
            odd = correlate(some, 2 * ch, 1)
            some = jnp.concatenate([ref[ch : 2 * ch, :], ref[ch3 + ch : ch3 + 2 * ch, :]], axis=0)
            keep(slice(0, ch), odd[0:ch])
            keep(slice(ch, 2 * ch), correlate(some, ch, 0))
            keep(slice(2 * ch, ch3), odd[ch : 2 * ch])
        else:
            keep(slice(0, ch3), correlate(ref[...], ch3, layer + 1))

        def store(t, line):
            for k in range(per):
                rs[layer, :, 9 * k + t, :] = line[k * n_own : (k + 1) * n_own]

        pairs(store)
        to_twin(rs.at[layer], ra.at[layer], ra_send.at[layer], ra_recv.at[layer])

    def send_extra(layer):
        at = LINEAR.index(layer)
        k = ch3 + 16
        stack_cols(hs, k, xh[layer])
        if layer == 0:
            even, odd = correlate(hs[...], k, 0), correlate(hs[...], k, 1)
            keep(slice(0, ch), odd[0:ch])
            keep(slice(ch, 2 * ch), even[ch : 2 * ch])
            keep(slice(2 * ch, ch3), odd[ch : 2 * ch])
            window = [odd[ch3 : ch3 + 1], even[ch3 + 1 : ch3 + 2], odd[ch3 + 1 : ch3 + 2]]
        else:
            both = correlate(hs[...], k, layer + 1)
            keep(slice(0, ch3), both[0:ch3])
            window = [both[ch3 + b : ch3 + b + 1] for b in range(3)]

        def store(t, line):
            for k in range(per):
                rx[at, :, 9 * k + t, :] = line[k * n_own : (k + 1) * n_own]

        pairs(store)
        for b in range(3):
            for a in range(3):
                one = window[b][:, a * ch : (a + 1) * ch]
                line = jnp.concatenate([one, one], axis=1)
                rx[at, :, 9 * per + 3 * a + b, :] = jnp.broadcast_to(line, (n_own, 2 * ch))
        to_twin(rx.at[at], rxa.at[at], rxa_send.at[at], rxa_recv.at[at])

    def pass_extra(layer):
        at = LINEAR.index(layer)
        send_parts(
            rx.at[at],
            rxa.at[at],
            rxp.at[at],
            rxbuf.at[at],
            rxa_recv.at[at],
            rx_send.at[at],
            rx_recv.at[at],
        )

    def finish(layer):
        scale, off, inv, by = affine[layer]
        d = xh[layer]
        y = scale * d + off
        xh[layer] = inv * (d - by)
        sig = jax.nn.sigmoid(y)
        yy[layer] = sig * (1.0 + y * (1.0 - sig))

    affine = []
    sigmas = {}
    act = None
    for layer in range(LAYERS):
        z = convolve(layer)
        sums = fold(z)
        m_loc = jnp.sum(sums, axis=1, keepdims=True) / entries_loc
        d = z - m_loc
        turned = jnp.concatenate([sums, fold(d * d)], axis=0).T
        row = jnp.sum(turned, axis=0, keepdims=True)
        row = jnp.where(lane < ch, row / entries_loc, row)
        send_row(st, layer + 1, row)
        xh[layer] = d
        if layer - 2 in LINEAR:
            pass_extra(layer - 2)
        if layer + 1 < LAYERS:
            weights(layer + 1)
        else:
            for s in range(sweeps):
                for r in range(h2):
                    at = s * plane + r * w2
                    cot_s[:, at : at + w2] = cot[s, :, r, :]
        if layer > 0:
            finish(layer - 1)
            if layer - 1 in LINEAR:
                send_extra(layer - 1)
        rows = wait_row(st, layer + 1)
        total = jnp.sum(rows, axis=0)
        means = total / float(n)
        dev = rows - means[None]
        spread = jnp.sum(dev * dev, axis=0) * entries_loc
        second = (total + pltpu.roll(spread, ch, axis=1)) / entries
        row = jnp.where(lane < ch, means, lax.rsqrt(second + EPS))
        mean_c, inv_c = columns(row)
        sq[layer, :, :] = jnp.broadcast_to(row, (8, 2 * ch))
        by = mean_c - m_loc
        scale = bn_cols[:, layer : layer + 1] * inv_c
        off = bn_cols[:, LAYERS + layer : LAYERS + layer + 1] - scale * by
        affine.append((scale, off, inv_c, by))
        y = scale * xh[layer] + off
        act = y * jax.nn.sigmoid(y)
        if layer + 1 < LAYERS:
            hi_lo = split(act)
            stack_rows(layer + 2, [(hi_lo, -1), (hi_lo, 0), (hi_lo, 1)])
        else:
            finish(layer)

    def backward(layer):
        w = wbs[layer - 1]
        big = dot(w, gs[0:ch3, :])
        v = big[0:ch3] + big[ch3 : 2 * ch3] + dot(w[0:ch3], gs[ch3 : 2 * ch3, :])
        return v[ch : 2 * ch] + down(v[0:ch], 1) + down(v[2 * ch : ch3], -1)

    u = cot_s[...]
    for layer in range(LAYERS - 1, -1, -1):
        gy = u * yy[layer]
        turned = jnp.concatenate([fold(gy), fold(gy * xh[layer])], axis=0).T
        rnd = 2 * LAYERS - layer
        send_row(st, rnd, jnp.sum(turned, axis=0, keepdims=True))
        if layer == LAYERS - 1:
            for s in range(sweeps):
                for r in range(h2):
                    at = s * plane + r * w2
                    feat[s, :, r, :] = act[:, at : at + w2]
        if layer in LINEAR:
            stack_cols(hs, ch3, gy, 2 if layer == 0 else 3)
            send_grad(hs.at[0 : 2 * ch3, :], layer)
        if layer + 1 < LAYERS and layer + 1 not in LINEAR:
            send_grad(gs, layer + 1)
        if layer in LINEAR:
            pass_on(layer)
        if layer == 0:
            share(LAYERS - 1)
        for done in range(LAYERS - 1, layer, -1):
            if done == layer + (1 if done in LINEAR else 2):
                add_parts(done)
        if layer + 1 < LAYERS and layer + 1 not in LINEAR:
            pass_on(layer + 1)
        row = jnp.sum(wait_row(st, rnd), axis=0)
        sigmas[layer] = row
        norms[0, layer : layer + 1, :] = row[:, ch : 2 * ch]
        norms[1, layer : layer + 1, :] = row[:, 0:ch]
        dy_c, dyx_c = columns(row / entries)
        gz = affine[layer][0] * (gy - dy_c - xh[layer] * dyx_c)
        if layer > 0:
            stack_cols(gs, ch3, gz)
            u = backward(layer)
    for dr in range(2):
        for dc in range(2):
            hi, lo = split(shift(down(gz, dr), dc))
            at = pl.ds((2 * dr + dc) * ch, ch)
            g4[0, at, :] = hi
            g4[1, at, :] = lo
    big = dot(wb0s[...], g4[0])
    u0 = big[0 : 4 * ch] + big[4 * ch :] + dot(wb0s[0 : 4 * ch, :], g4[1])
    for s in range(sweeps):
        total = None
        for k in range(4):
            hi, lo = split(u0[k * ch : (k + 1) * ch, s * plane : (s + 1) * plane])
            both = jnp.concatenate([hi, lo], axis=0)
            part = dot(both, onehot[s, :, k * plane : (k + 1) * plane], NT)
            total = part if total is None else total + part
        pgrad[s] = total[0:ch] + total[ch : 2 * ch]
    add_parts(0)

    def arrived(layer):
        on_core(0, lambda: landed(grads.at[layer], sh_recv.at[layer]))

    def unpack(layer):
        arrived(layer)
        for t in range(9):
            for k in range(per):
                part = grads[layer, :, 9 * k + t, :]
                out_g[t, k * n_own : (k + 1) * n_own, layer, :] = part

    def sent(ref, sem):
        by_role(lambda: landed(ref.at[pl.ds(0, n_own - 1)], sem), lambda: landed(ref, sem))

    def drain(layer):
        on_core(0, lambda: landed(ra.at[layer], ra_send.at[layer]))
        on_core(1, lambda: sent(rp.at[layer], rs_send.at[layer]))
        when_owner(lambda: landed(rbuf.at[layer, pl.ds(0, n_same - 1)], ag_send.at[layer]))

    for layer in range(LAYERS - 2, 0, -1):
        share(layer)
    for rnd in range(2 * LAYERS + 1):
        landed((st0.at[0] if rnd == 0 else st.at[rnd]).at[pl.ds(0, n - 1)], st_send.at[rnd])
    for at in range(len(LINEAR)):
        on_core(0, lambda: landed(rxa.at[at], rxa_send.at[at]))
        on_core(1, lambda: sent(rxp.at[at], rx_send.at[at]))
    for layer in range(LAYERS - 1, 0, -1):
        unpack(layer)
        drain(layer)
    share(0)
    drain(0)
    unpack(0)

    def shared():
        for layer in range(LAYERS):
            landed(grads.at[layer], sh_send.at[layer])

    on_core(1, shared)


def write_out(a, b, c, d, a_h, b_h, c_h, d_h, sem):
    pairs = [(b, b_h), (a, a_h), (d, d_h), (c, c_h)]
    copies = [pltpu.make_async_copy(x, y, sem.at[i]) for i, (x, y) in enumerate(pairs)]
    for x in copies:
        x.start()
    for x in copies:
        x.wait()


def per_device(
    n_rack,
    n_chip,
    points,
    counts,
    cells,
    pfn_weight,
    pfn_gain,
    pfn_bias,
    conv_weight,
    bn_gain,
    bn_bias,
    cotangent,
):
    sweeps, _, maxp, pill = points.shape
    ch = pfn_weight.shape[1]
    h2, w2 = cotangent.shape[2:]
    gh, gw = 2 * h2, 2 * w2
    n = n_rack * n_chip
    owners = ch // 2
    n_own = min(n // 2, owners)
    per = owners // n_own
    assert owners % n_own == 0 and n_rack % 2 == 0 and w2 == 128 and 2 * ch == 128
    pix = sweeps * h2 * w2
    ch3 = 3 * ch
    dims = (n_rack, n_chip, sweeps, maxp, gh, gw, pill, ch, owners)
    hbm = pl.BlockSpec(memory_space=pl.ANY)
    vmem = pl.BlockSpec(memory_space=pltpu.VMEM)
    extra = len(LINEAR)
    w4 = conv_weight.reshape(LAYERS, 9, owners, 2 * ch).transpose(1, 2, 0, 3)
    dma = pltpu.SemaphoreType.DMA
    outs = pl.pallas_call(
        functools.partial(kernel, dims),
        out_shape=(
            pltpu.VMEM((sweeps, ch, h2, w2), F32),
            pltpu.VMEM((9, owners, LAYERS, 2 * ch), F32),
            pltpu.VMEM((2, LAYERS, ch), F32),
            pltpu.VMEM((sweeps, ch, pill), F32),
        ),
        in_specs=[hbm] * 10,
        out_specs=(vmem,) * 4,
        scratch_shapes=[
            pltpu.VMEM((sweeps, 4, maxp, pill), F32),
            pltpu.VMEM((sweeps, pill), jnp.int32),
            pltpu.VMEM((sweeps, pill), jnp.int32),
            pltpu.VMEM((9, ch), F32),
            pltpu.SMEM((9, ch), F32),
            pltpu.VMEM((1, ch), F32),
            pltpu.VMEM((1, ch), F32),
            pltpu.VMEM((9, owners, LAYERS, 2 * ch), F32),
            pltpu.VMEM((LAYERS, ch), F32),
            pltpu.VMEM((LAYERS, ch), F32),
            pltpu.VMEM((sweeps, ch, h2, w2), F32),
            pltpu.VMEM((LAYERS + 1, 2, ch3, pix), BF16),
            pltpu.VMEM((2 * ch3, pix), BF16),
            pltpu.VMEM((2 * ch3 + 32, pix), BF16),
            pltpu.VMEM((2, ch3, 2 * ch), F32),
            pltpu.VMEM((2, ch3, 2 * ch), F32),
            pltpu.VMEM((LAYERS, 2 * ch3, ch3), BF16),
            pltpu.VMEM((LAYERS - 1, 2 * ch3, ch3), BF16),
            pltpu.VMEM((8 * ch, 4 * ch), BF16),
            pltpu.VMEM((2, 4 * ch, pix), BF16),
            pltpu.VMEM((sweeps, pill, gh * gw), BF16),
            pltpu.VMEM((32, 128), F32),
            pltpu.VMEM((ch, pix), F32),
            pltpu.VMEM((LAYERS, n_own, 9 * per, 2 * ch), F32),
            pltpu.VMEM((sweeps, ch, pill), F32),
            pltpu.VMEM((sweeps, ch, 8, pill), F32),
            pltpu.VMEM((ch, 8, 128), F32),
            pltpu.VMEM((LAYERS, ch, pix), F32),
            pltpu.VMEM((LAYERS, ch, pix), F32),
            pltpu.VMEM((1, n, 1, 4 * ch), F32),
            pltpu.VMEM((2 * LAYERS + 1, n, 1, 2 * ch), F32),
            pltpu.VMEM((LAYERS, n_own, 9 * per, 2 * ch), F32),
            pltpu.VMEM((LAYERS, n_own, 9 * per, 2 * ch), F32),
            pltpu.VMEM((LAYERS, n_own, 9 * per, 2 * ch), F32),
            pltpu.VMEM((LAYERS, n // 2, 9 * per, 2 * ch), F32),
            pltpu.VMEM((extra, n_own, 9 * per + 9, 2 * ch), F32),
            pltpu.VMEM((extra, n_own, 9 * per + 9, 2 * ch), F32),
            pltpu.VMEM((extra, n_own, 9 * per + 9, 2 * ch), F32),
            pltpu.VMEM((extra, n // 2, 9 * per + 9, 2 * ch), F32),
            dma((11,)),
            dma((2 * LAYERS + 1,)),
            dma((2 * LAYERS + 1,)),
            dma((LAYERS,)),
            dma((LAYERS,)),
            dma((LAYERS,)),
            dma((LAYERS,)),
            dma((extra,)),
            dma((extra,)),
            dma((extra,)),
            dma((extra,)),
            dma((LAYERS,)),
            dma((LAYERS,)),
            dma((LAYERS,)),
            dma((LAYERS,)),
        ],
        compiler_params=pltpu.CompilerParams(
            collective_id=0, has_side_effects=True, vmem_limit_bytes=56 * 1024 * 1024
        ),
    )(
        points,
        counts,
        cells,
        pfn_weight,
        pfn_gain.reshape(1, ch),
        pfn_bias.reshape(1, ch),
        w4,
        bn_gain,
        bn_bias,
        cotangent,
    )
    feat, out_g, norms, pgrad = pl.pallas_call(
        write_out,
        out_shape=tuple(jax.ShapeDtypeStruct(x.shape, x.dtype) for x in outs),
        in_specs=[vmem] * 4,
        out_specs=(hbm,) * 4,
        scratch_shapes=[dma((4,))],
    )(*[pltpu.with_memory_space_constraint(x, pltpu.VMEM) for x in outs])
    grads = out_g.transpose(2, 0, 1, 3).reshape(LAYERS, 9, ch * ch)
    return (feat, grads, norms, pgrad)


def solution(mesh):
    both = ("rack", "chip")
    return jax.shard_map(
        functools.partial(per_device, mesh.shape["rack"], mesh.shape["chip"]),
        mesh=mesh,
        in_specs=(
            P(both, None, None, None),
            P(both, None),
            P(both, None),
            P(),
            P(),
            P(),
            P(),
            P(),
            P(),
            P(both, None, None, None),
        ),
        out_specs=(
            P(both, None, None, None),
            P(),
            P(),
            P(both, None, None),
        ),
        check_vma=False,
    )
```
